32 devices in a mesh: dp: 4 (over z), tensor: 8 (over y, x, core).
Axes of the slice: x: 2, y: 2, z: 4, core: 2. Of those that a mesh axis runs over, the one named last changes fastest.
Arguments:
- embed_rows: bfloat16 [98304, 512], P('tensor', 'dp'), may hold values from -6 to 6
- head_rows: bfloat16 [98304, 512], P('tensor', 'dp'), may hold values from -6 to 6
- row_offsets: int32 [2, 9], replicated, may hold values from -2047 to 67583, as said below
- slot_table: int32 [1024], replicated, may hold values from 0 to 1023, as said below
- probe: bfloat16 [512, 1024], replicated, may hold values from -0.25 to 0.25
Outputs:
- stored: bfloat16 [1024, 128, 512], P(('dp', 'tensor'))
- sketch: float32 [1024, 128, 1024], P(('dp', 'tensor'))
The draws below stay inside these ranges and needn't reach their ends.
Inputs may be any that keep to these rules, and one draw needn't show every extreme that they name: row_offsets[m, 8] is row_offsets[m, 0] + 65536; every entry row_offsets[m, t] with t < 8 lies strictly within 2048 rows of t * 8192, and the distance 8192 // 4 - 1 is reached above and below among ranks 1 onward in every row of every draw; row_offsets[m, 0] is never 0, above 0 for one matrix and below 0 for the other. `slot_table`: A permutation of the 1024 block numbers. Devices along dp+tensor write 32 consecutive slots each; among one device's slots exactly 4 blocks come from each aligned range of 8192 vocabulary rows (rows t * 8192 onward of either matrix, both matrices together).
All inputs are finite; a program needn't handle non-finite values.
Results may differ from the reference program's by a relative error of at most 0.001.
Values may be sent and summed in bfloat16 or wider, within the bound.
A program may use at most 64 MiB of HBM per device.

```python
import jax
import jax.numpy as jnp
from jax import lax

R = 8192
PW = 1024
BLOCK = 128
CAP = 12288
C = 512
NBLK = 512
N_TENSOR = 8
DEVICES = 32


def draw_row_offsets(key, part):
    first, second, third, fourth, fifth = jax.random.split(key, 5)
    reach = R // 4 - 1
    inner = N_TENSOR - 1
    shifts = jax.random.randint(first, (2, inner), -reach, reach + 1)
    upper = jax.random.randint(second, (2,), 0, inner)
    lower = (upper + 1 + jax.random.randint(third, (2,), 0, inner - 1)) % inner
    column = jnp.arange(inner)[None, :]
    shifts = jnp.where(column == upper[:, None], reach, shifts)
    shifts = jnp.where(column == lower[:, None], -reach, shifts)
    interior = jnp.arange(1, N_TENSOR)[None, :] * R + shifts
    size = jax.random.randint(fourth, (2,), 1, reach + 1)
    flip = jax.random.randint(fifth, (), 0, 2)
    signs = jnp.where(jnp.arange(2) == flip, 1, -1)
    starts = (signs * size).astype(jnp.int32)[:, None]
    ends = starts + R * N_TENSOR
    return jnp.concatenate([starts, interior.astype(jnp.int32), ends], axis=1).astype(jnp.int32)


def draw_slot_table(key, part):
    first, second = jax.random.split(key)
    per_rank = R // BLOCK
    total_blocks = per_rank * N_TENSOR
    slot_count = 2 * total_blocks // DEVICES
    shuffled = jax.random.permutation(first, DEVICES).astype(jnp.int32)
    source = (shuffled[:, None] + jnp.arange(slot_count, dtype=jnp.int32)[None, :]) % N_TENSOR
    flat_source = source.reshape(-1)
    slot_total = DEVICES * slot_count
    noise = jax.random.permutation(second, slot_total).astype(jnp.int32)
    ordering = jnp.argsort(flat_source * slot_total + noise)
    within = jnp.arange(slot_total, dtype=jnp.int32) % (2 * per_rank)
    local_block = jnp.zeros((slot_total,), jnp.int32).at[ordering].set(within)
    result = local_block // per_rank * total_blocks + flat_source * per_rank + local_block % per_rank
    return result.astype(jnp.int32)


def steps_of(own_key, extent, pieces, least, high):
    level = 1.0
    for position, parts in pieces:
        draws = jax.random.uniform(jax.random.fold_in(jax.random.fold_in(own_key, 6), position), (parts,), jnp.float32, least / len(pieces), high / len(pieces))
        level = level * jnp.repeat(jnp.exp(draws), extent[position] // parts).reshape((-1,) + (1,) * (len(extent) - 1 - position))
    return level


def normal_values(own_key, extent, scale, bound, cuts=(), kind=jnp.bfloat16):
    gain = steps_of(own_key, extent, cuts, -0.22, 0.18) if cuts else 1.0
    array = jax.random.normal(own_key, extent, jnp.float32) * scale * gain
    return jnp.minimum(jnp.maximum(array, -bound), bound).astype(kind)


def setup_inputs(seed: int = 0) -> dict:
    seeds = jax.random.split(jax.random.key(seed), 6)
    embed_rows = normal_values(seeds[0], (N_TENSOR * CAP, C), 1.0, 6.0, ((0, 8), (1, 4)))
    head_rows = normal_values(seeds[1], (N_TENSOR * CAP, C), 1.0, 6.0, ((0, 8), (1, 4)))
    row_offsets = draw_row_offsets(jax.random.fold_in(seeds[5], 71), 0)
    slot_table = draw_slot_table(jax.random.fold_in(seeds[5], 71), 0)
    probe = normal_values(seeds[4], (C, PW), C ** -0.5, 0.25)
    return dict(embed_rows=embed_rows, head_rows=head_rows, row_offsets=row_offsets, slot_table=slot_table, probe=probe)


def assemble(buffer, offsets):
    vocab_rows = jnp.arange(R * N_TENSOR, dtype=jnp.int32)
    unwrapped = jnp.where(vocab_rows < offsets[0], vocab_rows + R * N_TENSOR,
                          jnp.where(vocab_rows >= offsets[N_TENSOR], vocab_rows - R * N_TENSOR, vocab_rows)).astype(jnp.int32)
    owner = jnp.sum((offsets[1:N_TENSOR][None, :] <= unwrapped[:, None]).astype(jnp.int32), axis=1).astype(jnp.int32)
    source_row = (owner * CAP + unwrapped - offsets[owner]).astype(jnp.int32)
    return buffer[source_row]


def reference(embed_rows, head_rows, row_offsets, slot_table, probe):
    whole = jnp.concatenate([assemble(embed_rows, row_offsets[0]), assemble(head_rows, row_offsets[1])], axis=0)
    blocks = whole.reshape(2 * NBLK, BLOCK, C)
    stored = blocks[slot_table]
    sketch = jnp.dot(stored.reshape(-1, C).astype(jnp.float32), probe.astype(jnp.float32),
                     precision=lax.Precision.HIGHEST, preferred_element_type=jnp.float32)
    return stored, sketch.reshape(2 * NBLK, BLOCK, PW)
```

```python
import functools

import jax
import jax.numpy as jnp
from jax import lax
from jax.experimental import pallas as pl
from jax.experimental.pallas import tpu as pltpu
from jax.sharding import PartitionSpec as P

MESH = pl.DeviceIdType.MESH
AXES = ("dp", "tensor")
BLOCK = 128
TILE = 16
WINDOW = 256
MIB = 1 << 20


def tile_of(value):
    return lax.shift_right_arithmetic(value, 4)


def tail_begin(offset, rank, span, height):
    return jnp.clip((rank + 1) * span - offset, 0, height - span // 4 - 1)


def selector(offset):
    row = lax.broadcasted_iota(jnp.int32, (BLOCK, WINDOW), 0)
    column = lax.broadcasted_iota(jnp.int32, (BLOCK, WINDOW), 1)
    return jnp.where(column - row == offset, 1.0, 0.0).astype(jnp.bfloat16)


def moved(offset, window):
    return jnp.dot(selector(offset), window, preferred_element_type=jnp.float32)


def plan_kernel(n_tensor, per_rank, first_turns, offsets_ref, grid_ref, picks_ref, where_ref, late_ref):
    me = lax.axis_index("tensor")
    span = per_rank * BLOCK
    grid = grid_ref[...]
    devices, slots = grid.shape
    total = n_tensor * per_rank
    matrix = (grid >= total).astype(jnp.int32)
    within = grid - matrix * total
    source = lax.shift_right_logical(within, per_rank.bit_length() - 1)
    block = within - source * per_rank
    first = block * BLOCK
    far = jnp.zeros(grid.shape, jnp.int32)
    for m in range(2):
        for t in range(n_tensor):
            if t % 2 == 0:
                touched = first < offsets_ref[m, t] - t * span
            else:
                touched = first + BLOCK > offsets_ref[m, t + 1] - t * span
            here = (source == t) & (matrix == m)
            far = far + jnp.where(here & touched, 1, 0)
    lane = lax.broadcasted_iota(jnp.int32, grid.shape, 1)
    key = far * slots + lane
    turn = jnp.zeros(grid.shape, jnp.int32)
    for s in range(slots):
        ahead = (source[:, s : s + 1] == source) & (key[:, s : s + 1] < key)
        turn = turn + jnp.where(ahead, 1, 0)
    most = slots // n_tensor
    local = matrix * per_rank + block
    column = lax.broadcasted_iota(jnp.int32, picks_ref.shape, 1)
    picks = jnp.zeros(picks_ref.shape, jnp.int32)
    for j in range(most):
        chosen = jnp.where((source == me) & (turn == j), local, 0)
        picks = jnp.where(column == j, jnp.sum(chosen, axis=1, keepdims=True), picks)
    picks_ref[...] = picks
    where_ref[...] = source * most + turn
    wrong = jnp.where(turn < first_turns, far, 0)
    late_ref[...] = jnp.sum(jnp.sum(wrong, axis=1, keepdims=True), axis=0, keepdims=True)


def exchange_kernel(n_data, n_tensor, per_rank, first_turns, picks_ref, offsets_ref, embed_ref, head_ref,
                    incoming_ref, again_ref, rows, trail, near, far, ready, rest,
                    load_sems, edge_send, edge_recv, send_sems, recv_sems):
    data, rank = lax.axis_index("dp"), lax.axis_index("tensor")
    devices = n_data * n_tensor
    me = data * n_tensor + rank
    span = per_rank * BLOCK
    height = rows.shape[1] * TILE
    edge = trail.shape[1]
    most = incoming_ref.shape[0] // devices
    last_turns = most - first_turns
    even = rank % 2 == 0
    near_rank = jnp.where(even, rank + 1, rank - 1)
    far_rank = jnp.where(even, (rank + n_tensor - 1) % n_tensor, (rank + 1) % n_tensor)
    left = (rank + n_tensor - 1) % n_tensor

    loads = [
        pltpu.make_async_copy(buffer, rows.at[m], load_sems.at[m])
        for m, buffer in enumerate((embed_ref, head_ref))
    ]
    for load in loads:
        load.start()

    def peer(k):
        return (data + k % n_data) % n_data, (rank + k // n_data) % n_tensor

    barrier = pltpu.get_barrier_semaphore()

    def greet(k, carry):
        d, t = peer(k)
        pl.semaphore_signal(barrier, inc=1, device_id=(d, t), device_id_type=MESH)
        return carry

    lax.fori_loop(1, devices, greet, 0)

    for load in loads:
        load.wait()

    def fill(i, carry):
        for m in range(2):
            trail[m, i] = rows[m, tile_of(tail_begin(offsets_ref[m, rank], rank, span, height)) + i]
        return carry

    lax.fori_loop(0, edge, fill, 0)
    pl.semaphore_wait(barrier, devices - 1)

    lead = rows.at[:, pl.ds(0, edge)]

    def edge_copy(source, target, which, t):
        return pltpu.make_async_remote_copy(
            src_ref=source, dst_ref=target, send_sem=edge_send.at[which], recv_sem=edge_recv.at[which],
            device_id=(data, t), device_id_type=MESH,
        )

    @pl.when(even)
    def _():
        edge_copy(trail, near, 0, near_rank).start()
        edge_copy(lead, far, 1, far_rank).start()

    @pl.when(jnp.logical_not(even))
    def _():
        edge_copy(lead, near, 0, near_rank).start()
        edge_copy(trail, far, 1, far_rank).start()

    row = lax.broadcasted_iota(jnp.int32, (BLOCK, rows.shape[3]), 0)

    def window(buffer, m, start):
        base = jnp.clip(tile_of(start), 0, buffer.shape[1] - WINDOW // TILE)
        tiles = [buffer[m, base + i] for i in range(WINDOW // TILE)]
        return jnp.concatenate(tiles, axis=0), start - base * TILE

    def gathered(dest, j, with_far):
        number = picks_ref[dest, j]
        m = (number >= per_rank).astype(jnp.int32)
        first = (number - m * per_rank) * BLOCK
        low = jnp.where(m == 0, offsets_ref[0, rank], offsets_ref[1, rank]) - rank * span - first
        high = jnp.where(m == 0, offsets_ref[0, rank + 1], offsets_ref[1, rank + 1]) - rank * span - first
        left_begin = tail_begin(jnp.where(m == 0, offsets_ref[0, left], offsets_ref[1, left]), left, span, height)
        own, own_offset = window(rows, m, -low)
        from_left = first + left_begin - tile_of(left_begin) * TILE
        from_right = -high
        piece, offset = window(near, m, jnp.where(even, from_right, from_left))
        if with_far:
            use_far = jnp.where(even, low > 0, high < BLOCK)
            other, other_offset = window(far, m, jnp.where(even, from_left, from_right))
            piece = jnp.where(use_far, other, piece)
            offset = jnp.where(use_far, other_offset, offset)
        kept = moved(own_offset, own)
        patch = moved(offset, piece)
        return jnp.where((row >= low) & (row < high), kept, patch).astype(rows.dtype)

    def send(phase, staged, count, base, d, t):
        to = d * n_tensor + t
        return pltpu.make_async_remote_copy(
            src_ref=staged.at[pl.ds(to * count, count)],
            dst_ref=incoming_ref.at[pl.ds(me * most + base, count)],
            send_sem=send_sems.at[phase, to], recv_sem=recv_sems.at[phase, me],
            device_id=(d, t), device_id_type=MESH,
        )

    def wait_edge(which, target):
        copy = edge_copy(trail, target, which, near_rank)
        copy.wait_recv()

    def phase_of(phase, staged, count, base, with_far):
        for j in range(count):
            incoming_ref[me * most + base + j] = gathered(me, base + j, with_far)

        def one(k, carry):
            d, t = peer(k)
            to = d * n_tensor + t
            for j in range(count):
                staged[to * count + j] = gathered(to, base + j, with_far)

            @pl.when(k > 1)
            def _():
                send(phase, staged, count, base, *peer(k - 1)).start()

            return carry

        lax.fori_loop(1, devices, one, 0)
        send(phase, staged, count, base, *peer(devices - 1)).start()

    wait_edge(0, near)
    if first_turns:
        phase_of(0, ready, first_turns, 0, False)
    wait_edge(1, far)
    phase_of(1, rest, last_turns, first_turns, True)

    if first_turns:
        def redo(to, carry):
            for j in range(first_turns):
                again_ref[to * first_turns + j] = gathered(to, j, True)
            return carry

        lax.fori_loop(0, devices, redo, 0)
    else:
        again_ref[...] = jnp.zeros_like(again_ref)

    edge_copy(trail, near, 0, near_rank).wait_send()
    edge_copy(trail, far, 1, far_rank).wait_send()

    def finish_phase(phase, staged, count, base):
        def drain(k, carry):
            d, t = peer(k)
            send(phase, staged, count, base, d, t).wait_send()
            pltpu.make_async_remote_copy(
                src_ref=staged.at[pl.ds(me * count, count)],
                dst_ref=incoming_ref.at[pl.ds((d * n_tensor + t) * most + base, count)],
                send_sem=send_sems.at[phase, me], recv_sem=recv_sems.at[phase, d * n_tensor + t],
                device_id=(d, t), device_id_type=MESH,
            ).wait_recv()
            return carry

        lax.fori_loop(1, devices, drain, 0)

    if first_turns:
        finish_phase(0, ready, first_turns, 0)
    finish_phase(1, rest, last_turns, first_turns)


def finish_kernel(n_data, n_tensor, per_step, where_ref, incoming_ref, probe_ref, stored_ref, sketch_ref):
    width = incoming_ref.shape[2]
    stride = incoming_ref.shape[0] // n_data
    me = lax.axis_index("dp") * n_tensor + lax.axis_index("tensor")
    step = pl.program_id(0)
    for q in range(per_step):
        base = where_ref[me, step * per_step + q]
        for d in range(n_data):
            stored_ref[q, :, d * width : (d + 1) * width] = incoming_ref[base + d * stride]
    rows = stored_ref[...].reshape(per_step * BLOCK, n_data * width)
    product = jnp.dot(rows, probe_ref[...], preferred_element_type=jnp.float32)
    sketch_ref[...] = product.reshape(sketch_ref.shape)


def plan(row_offsets, slot_grid, n_tensor, per_rank, first_turns):
    devices, slots = slot_grid.shape
    vmem = pl.BlockSpec(memory_space=pltpu.VMEM)
    return pl.pallas_call(
        functools.partial(plan_kernel, n_tensor, per_rank, first_turns),
        in_specs=[pl.BlockSpec(memory_space=pltpu.SMEM), vmem],
        out_specs=[vmem, vmem, vmem],
        out_shape=[
            jax.ShapeDtypeStruct((devices, slots // n_tensor), jnp.int32),
            jax.ShapeDtypeStruct((devices, slots), jnp.int32),
            jax.ShapeDtypeStruct((1, 1), jnp.int32),
        ],
        name="plan",
    )(row_offsets, slot_grid)


def exchange(picks, row_offsets, embed_rows, head_rows, n_data, n_tensor, per_rank, first_turns):
    height, width = embed_rows.shape
    kind = embed_rows.dtype
    devices = n_data * n_tensor
    most = picks.shape[1]
    edge = per_rank * BLOCK // 4 // TILE + 1
    smem = pl.BlockSpec(memory_space=pltpu.SMEM)
    vmem = pl.BlockSpec(memory_space=pltpu.VMEM)
    hbm = pl.BlockSpec(memory_space=pltpu.HBM)
    return pl.pallas_call(
        functools.partial(exchange_kernel, n_data, n_tensor, per_rank, first_turns),
        in_specs=[smem, smem, hbm, hbm],
        out_specs=[vmem, vmem],
        out_shape=[
            jax.ShapeDtypeStruct((devices * most, BLOCK, width), kind),
            jax.ShapeDtypeStruct((devices * max(first_turns, 1), BLOCK, width), kind),
        ],
        scratch_shapes=[
            pltpu.VMEM((2, height // TILE, TILE, width), kind),
            pltpu.VMEM((2, edge, TILE, width), kind),
            pltpu.VMEM((2, edge, TILE, width), kind),
            pltpu.VMEM((2, edge, TILE, width), kind),
            pltpu.VMEM((devices * max(first_turns, 1), BLOCK, width), kind),
            pltpu.VMEM((devices * (most - first_turns), BLOCK, width), kind),
            pltpu.SemaphoreType.DMA((2,)),
            pltpu.SemaphoreType.DMA((2,)),
            pltpu.SemaphoreType.DMA((2,)),
            pltpu.SemaphoreType.DMA((2, devices)),
            pltpu.SemaphoreType.DMA((2, devices)),
        ],
        compiler_params=pltpu.CompilerParams(
            collective_id=0, has_side_effects=True, vmem_limit_bytes=32 * MIB
        ),
        name="exchange",
    )(picks, row_offsets, embed_rows.reshape(-1, TILE, width), head_rows.reshape(-1, TILE, width))


def finish(where, incoming, probe, n_data, n_tensor):
    columns, sketch_width = probe.shape
    slot_count = where.shape[1]
    per_step = 4
    return pl.pallas_call(
        functools.partial(finish_kernel, n_data, n_tensor, per_step),
        grid_spec=pltpu.PrefetchScalarGridSpec(
            num_scalar_prefetch=1,
            grid=(slot_count // per_step,),
            in_specs=[
                pl.BlockSpec(memory_space=pltpu.VMEM),
                pl.BlockSpec(memory_space=pltpu.VMEM),
            ],
            out_specs=[
                pl.BlockSpec((per_step, BLOCK, columns), lambda i, *_: (i, 0, 0)),
                pl.BlockSpec((per_step, BLOCK, sketch_width), lambda i, *_: (i, 0, 0)),
            ],
        ),
        out_shape=[
            jax.ShapeDtypeStruct((slot_count, BLOCK, columns), incoming.dtype),
            jax.ShapeDtypeStruct((slot_count, BLOCK, sketch_width), jnp.float32),
        ],
        compiler_params=pltpu.CompilerParams(
            dimension_semantics=("arbitrary",), vmem_limit_bytes=32 * MIB
        ),
        name="finish",
    )(where, incoming, probe)


def shards(embed_rows, head_rows, row_offsets, slot_table, probe):
    n_data, n_tensor = lax.axis_size("dp"), lax.axis_size("tensor")
    devices = n_data * n_tensor
    per_rank = slot_table.shape[0] // (2 * n_tensor)
    slots = slot_table.shape[0] // devices
    most = slots // n_tensor
    first_turns = most // 4
    picks, where, late = plan(row_offsets, slot_table.reshape(devices, slots), n_tensor, per_rank, first_turns)
    incoming, again = exchange(picks, row_offsets, embed_rows, head_rows, n_data, n_tensor, per_rank, first_turns)

    def ended(where, incoming, again, probe):
        return tuple(finish(where, incoming, probe, n_data, n_tensor))

    def resent(where, incoming, again, probe):
        fresh = lax.all_to_all(again, AXES, split_axis=0, concat_axis=0, tiled=True)
        shape = incoming.shape
        fresh = fresh.reshape((devices, first_turns) + shape[1:])
        held = incoming.reshape((devices, most) + shape[1:])
        whole = jnp.concatenate([fresh, held[:, first_turns:]], axis=1).reshape(shape)
        return ended(where, whole, again, probe)

    if not first_turns:
        return ended(where, incoming, again, probe)
    return lax.cond(late[0, 0] == 0, ended, resent, where, incoming, again, probe)


def solution(mesh):
    return jax.shard_map(
        shards,
        mesh=mesh,
        in_specs=(P("tensor", "dp"), P("tensor", "dp"), P(), P(), P()),
        out_specs=(P(AXES, None, None), P(AXES, None, None)),
        check_vma=False,
    )
```

```python
import functools

import jax
import jax.numpy as jnp
from jax import lax
from jax.experimental import pallas as pl
from jax.experimental.pallas import tpu as pltpu
from jax.sharding import PartitionSpec as P

MESH = pl.DeviceIdType.MESH
AXES = ("dp", "tensor")
BLOCK = 128
TILE = 16
WINDOW = 256
LANES = 128
MIB = 1 << 20


def tile_of(value):
    return lax.shift_right_arithmetic(value, 4)


def tail_begin(offset, rank, span, height):
    return jnp.clip((rank + 1) * span - offset, 0, height - span // 4 - 1)


def selector(offset):
    row = lax.broadcasted_iota(jnp.int32, (BLOCK, WINDOW), 0)
    column = lax.broadcasted_iota(jnp.int32, (BLOCK, WINDOW), 1)
    return jnp.where(column - row == offset, 1.0, 0.0).astype(jnp.bfloat16)


def moved(offset, window):
    return jnp.dot(selector(offset), window, preferred_element_type=jnp.float32)


def plan_kernel(n_tensor, per_rank, slots, first_turns, offsets_ref, grid_ref, picks_ref, where_ref, late_ref):
    me = lax.axis_index("tensor")
    span = per_rank * BLOCK
    grid = grid_ref[...]
    total = n_tensor * per_rank
    matrix = (grid >= total).astype(jnp.int32)
    within = grid - matrix * total
    source = lax.shift_right_logical(within, per_rank.bit_length() - 1)
    block = within - source * per_rank
    first = block * BLOCK
    far = jnp.zeros(grid.shape, jnp.int32)
    for m in range(2):
        for t in range(n_tensor):
            if t % 2 == 0:
                touched = first < offsets_ref[m, t] - t * span
            else:
                touched = first + BLOCK > offsets_ref[m, t + 1] - t * span
            here = (source == t) & (matrix == m)
            far = far + jnp.where(here & touched, 1, 0)
    lane = lax.broadcasted_iota(jnp.int32, grid.shape, 1)
    slot = lane % slots
    code = source * 2 + far
    turn = jnp.zeros(grid.shape, jnp.int32)
    for k in range(1, slots):
        behind = pltpu.roll(code, k, 1)
        ahead = pltpu.roll(code, LANES - k, 1)
        same = (behind == code) | (behind == code - far)
        turn = turn + jnp.where((slot >= k) & same, 1, 0)
        turn = turn + jnp.where((slot + k < slots) & (far == 1) & (ahead == code - 1), 1, 0)
    most = slots // n_tensor
    local = matrix * per_rank + block
    group_row = lax.broadcasted_iota(jnp.int32, (LANES, LANES), 0) // slots
    group_column = lax.broadcasted_iota(jnp.int32, (LANES, LANES), 1)
    picks = jnp.zeros(grid.shape, jnp.float32)
    for j in range(most):
        chosen = jnp.where((source == me) & (turn == j), local, 0).astype(jnp.float32)
        spread = jnp.where(group_column == group_row * most + j, 1.0, 0.0)
        picks = picks + jnp.dot(chosen, spread, preferred_element_type=jnp.float32)
    picks_ref[...] = picks.astype(jnp.int32)
    where_ref[...] = source * most + turn
    wrong = jnp.where(turn < first_turns, far, 0)
    late_ref[...] = jnp.sum(jnp.sum(wrong, axis=1, keepdims=True), axis=0, keepdims=True)


def exchange_kernel(n_data, n_tensor, per_rank, first_turns, picks_ref, offsets_ref, embed_ref, head_ref,
                    incoming_ref, again_ref, rows, trail, near, far, ready, rest, patched,
                    load_sems, save_sem, edge_send, edge_recv, send_sems, recv_sems):
    data, rank = lax.axis_index("dp"), lax.axis_index("tensor")
    devices = n_data * n_tensor
    me = data * n_tensor + rank
    span = per_rank * BLOCK
    height = rows.shape[1] * TILE
    edge = trail.shape[1]
    most = incoming_ref.shape[0] // devices
    last_turns = most - first_turns
    groups = LANES // (most * n_tensor)
    even = rank % 2 == 0
    near_rank = jnp.where(even, rank + 1, rank - 1)
    far_rank = jnp.where(even, (rank + n_tensor - 1) % n_tensor, (rank + 1) % n_tensor)
    left = (rank + n_tensor - 1) % n_tensor

    loads = [
        pltpu.make_async_copy(buffer, rows.at[m], load_sems.at[m])
        for m, buffer in enumerate((embed_ref, head_ref))
    ]
    for load in loads:
        load.start()

    def peer(k):
        return (data + k % n_data) % n_data, (rank + k // n_data) % n_tensor

    barrier = pltpu.get_barrier_semaphore()

    def greet(k, carry):
        d, t = peer(k)
        pl.semaphore_signal(barrier, inc=1, device_id=(d, t), device_id_type=MESH)
        return carry

    lax.fori_loop(1, devices, greet, 0)

    for load in loads:
        load.wait()

    def fill(i, carry):
        for m in range(2):
            trail[m, i] = rows[m, tile_of(tail_begin(offsets_ref[m, rank], rank, span, height)) + i]
        return carry

    lax.fori_loop(0, edge, fill, 0)
    pl.semaphore_wait(barrier, devices - 1)

    lead = rows.at[:, pl.ds(0, edge)]

    def edge_copy(source, target, which, t):
        return pltpu.make_async_remote_copy(
            src_ref=source, dst_ref=target, send_sem=edge_send.at[which], recv_sem=edge_recv.at[which],
            device_id=(data, t), device_id_type=MESH,
        )

    @pl.when(even)
    def _():
        edge_copy(trail, near, 0, near_rank).start()
        edge_copy(lead, far, 1, far_rank).start()

    @pl.when(jnp.logical_not(even))
    def _():
        edge_copy(lead, near, 0, near_rank).start()
        edge_copy(trail, far, 1, far_rank).start()

    row = lax.broadcasted_iota(jnp.int32, (BLOCK, rows.shape[3]), 0)

    def window(buffer, m, start):
        base = jnp.clip(tile_of(start), 0, buffer.shape[1] - WINDOW // TILE)
        tiles = [buffer[m, base + i] for i in range(WINDOW // TILE)]
        return jnp.concatenate(tiles, axis=0), start - base * TILE

    def gathered(dest, j, with_far):
        number = picks_ref[dest // groups, dest % groups * most + j]
        m = (number >= per_rank).astype(jnp.int32)
        first = (number - m * per_rank) * BLOCK
        low = jnp.where(m == 0, offsets_ref[0, rank], offsets_ref[1, rank]) - rank * span - first
        high = jnp.where(m == 0, offsets_ref[0, rank + 1], offsets_ref[1, rank + 1]) - rank * span - first
        left_begin = tail_begin(jnp.where(m == 0, offsets_ref[0, left], offsets_ref[1, left]), left, span, height)
        own, own_offset = window(rows, m, -low)
        from_left = first + left_begin - tile_of(left_begin) * TILE
        from_right = -high
        piece, offset = window(near, m, jnp.where(even, from_right, from_left))
        if with_far:
            use_far = jnp.where(even, low > 0, high < BLOCK)
            other, other_offset = window(far, m, jnp.where(even, from_left, from_right))
            piece = jnp.where(use_far, other, piece)
            offset = jnp.where(use_far, other_offset, offset)
        kept = moved(own_offset, own)
        patch = moved(offset, piece)
        return jnp.where((row >= low) & (row < high), kept, patch).astype(rows.dtype)

    def send(phase, staged, count, base, d, t):
        to = d * n_tensor + t
        return pltpu.make_async_remote_copy(
            src_ref=staged.at[pl.ds(to * count, count)],
            dst_ref=incoming_ref.at[pl.ds(me * most + base, count)],
            send_sem=send_sems.at[phase, to], recv_sem=recv_sems.at[phase, me],
            device_id=(d, t), device_id_type=MESH,
        )

    def keep(phase, staged, count, base):
        return pltpu.make_async_copy(
            staged.at[pl.ds(me * count, count)], incoming_ref.at[pl.ds(me * most + base, count)], load_sems.at[phase]
        )

    def wait_edge(which, target):
        copy = edge_copy(trail, target, which, near_rank)
        copy.wait_recv()

    def phase_of(phase, staged, count, base, with_far):
        for j in range(count):
            staged[me * count + j] = gathered(me, base + j, with_far)

        def one(k, carry):
            d, t = peer(k)
            to = d * n_tensor + t
            for j in range(count):
                staged[to * count + j] = gathered(to, base + j, with_far)

            @pl.when(k > 1)
            def _():
                send(phase, staged, count, base, *peer(k - 1)).start()

            return carry

        lax.fori_loop(1, devices, one, 0)
        send(phase, staged, count, base, *peer(devices - 1)).start()
        keep(phase, staged, count, base).start()

    wait_edge(0, near)
    if first_turns:
        phase_of(0, ready, first_turns, 0, False)
    wait_edge(1, far)
    phase_of(1, rest, last_turns, first_turns, True)

    if first_turns:
        def redo(to, carry):
            for j in range(first_turns):
                patched[to * first_turns + j] = gathered(to, j, True)
            return carry

        lax.fori_loop(0, devices, redo, 0)
        save = pltpu.make_async_copy(patched, again_ref, save_sem)
        save.start()
        save.wait()

    edge_copy(trail, near, 0, near_rank).wait_send()
    edge_copy(trail, far, 1, far_rank).wait_send()

    def finish_phase(phase, staged, count, base):
        def drain(k, carry):
            d, t = peer(k)
            send(phase, staged, count, base, d, t).wait_send()
            pltpu.make_async_remote_copy(
                src_ref=staged.at[pl.ds(me * count, count)],
                dst_ref=incoming_ref.at[pl.ds((d * n_tensor + t) * most + base, count)],
                send_sem=send_sems.at[phase, me], recv_sem=recv_sems.at[phase, d * n_tensor + t],
                device_id=(d, t), device_id_type=MESH,
            ).wait_recv()
            return carry

        lax.fori_loop(1, devices, drain, 0)
        keep(phase, staged, count, base).wait()

    if first_turns:
        finish_phase(0, ready, first_turns, 0)
    finish_phase(1, rest, last_turns, first_turns)


def finish_kernel(n_data, n_tensor, where_ref, incoming_ref, probe_ref, stored_ref, sketch_ref,
                  slot_of, stored, sketch, load_sems, stored_sems, sketch_sems):
    width = incoming_ref.shape[2]
    slots = stored_ref.shape[0]
    most, groups = slots // n_tensor, LANES // slots
    buffers = sketch.shape[0]
    me = lax.axis_index("dp") * n_tensor + lax.axis_index("tensor")
    for t in range(n_tensor):
        for d in range(n_data):
            pltpu.make_async_copy(
                incoming_ref.at[pl.ds((d * n_tensor + t) * most, most)],
                stored.at[t, :, :, pl.ds(d * width, width)],
                load_sems.at[t, d],
            ).start()
    for s in range(slots):
        slot_of[where_ref[me // groups, me % groups * slots + s]] = s

    def writes(t):
        b = t % buffers
        copies = []
        for r in range(most):
            slot = slot_of[t * most + r]
            copies.append(pltpu.make_async_copy(sketch.at[b, r], sketch_ref.at[slot], sketch_sems.at[b, r]))
            copies.append(pltpu.make_async_copy(stored.at[t, r], stored_ref.at[slot], stored_sems.at[t, r]))
        return copies

    for t in range(n_tensor):
        b = t % buffers
        for d in range(n_data):
            pltpu.make_async_copy(
                incoming_ref.at[pl.ds((d * n_tensor + t) * most, most)],
                stored.at[t, :, :, pl.ds(d * width, width)],
                load_sems.at[t, d],
            ).wait()
        if t >= buffers:
            for write in writes(t - buffers):
                write.wait()
        rows = stored[t].reshape(most * BLOCK, n_data * width)
        product = jnp.dot(rows, probe_ref[...], preferred_element_type=jnp.float32)
        sketch[b] = product.reshape(sketch.shape[1:])
        for write in writes(t):
            write.start()
    for t in range(max(n_tensor - buffers, 0), n_tensor):
        for write in writes(t):
            write.wait()


def patch_kernel(n_data, n_tensor, first_turns, where_ref, fresh_ref, probe_ref, old_stored_ref, old_sketch_ref,
                 stored_ref, sketch_ref, stored, sketch, sems):
    width = fresh_ref.shape[2]
    slots = stored_ref.shape[0]
    most, groups = slots // n_tensor, LANES // slots
    me = lax.axis_index("dp") * n_tensor + lax.axis_index("tensor")

    def one(slot, carry):
        base = where_ref[me // groups, me % groups * slots + slot]
        turn = base % most

        @pl.when(turn < first_turns)
        def _():
            for d in range(n_data):
                held = (base // most + d * n_tensor) * first_turns + turn
                stored[:, d * width : (d + 1) * width] = fresh_ref[held]
            sketch[...] = jnp.dot(stored[...], probe_ref[...], preferred_element_type=jnp.float32)
            writes = (
                pltpu.make_async_copy(stored, stored_ref.at[slot], sems.at[0]),
                pltpu.make_async_copy(sketch, sketch_ref.at[slot], sems.at[1]),
            )
            for write in writes:
                write.start()
            for write in writes:
                write.wait()

        return carry

    lax.fori_loop(0, slots, one, 0)


def plan(row_offsets, grid, n_tensor, per_rank, slots, first_turns):
    vmem = pl.BlockSpec(memory_space=pltpu.VMEM)
    return pl.pallas_call(
        functools.partial(plan_kernel, n_tensor, per_rank, slots, first_turns),
        in_specs=[pl.BlockSpec(memory_space=pltpu.SMEM), vmem],
        out_specs=[vmem, vmem, vmem],
        out_shape=[
            jax.ShapeDtypeStruct(grid.shape, jnp.int32),
            jax.ShapeDtypeStruct(grid.shape, jnp.int32),
            jax.ShapeDtypeStruct((1, 1), jnp.int32),
        ],
        name="plan",
    )(row_offsets, grid)


def exchange(picks, row_offsets, embed_rows, head_rows, n_data, n_tensor, per_rank, most, first_turns):
    height, width = embed_rows.shape
    kind = embed_rows.dtype
    devices = n_data * n_tensor
    edge = per_rank * BLOCK // 4 // TILE + 1
    smem = pl.BlockSpec(memory_space=pltpu.SMEM)
    vmem = pl.BlockSpec(memory_space=pltpu.VMEM)
    hbm = pl.BlockSpec(memory_space=pltpu.HBM)
    return pl.pallas_call(
        functools.partial(exchange_kernel, n_data, n_tensor, per_rank, first_turns),
        in_specs=[smem, smem, hbm, hbm],
        out_specs=[hbm, hbm],
        out_shape=[
            jax.ShapeDtypeStruct((devices * most, BLOCK, width), kind),
            jax.ShapeDtypeStruct((devices * max(first_turns, 1), BLOCK, width), kind),
        ],
        scratch_shapes=[
            pltpu.VMEM((2, height // TILE, TILE, width), kind),
            pltpu.VMEM((2, edge, TILE, width), kind),
            pltpu.VMEM((2, edge, TILE, width), kind),
            pltpu.VMEM((2, edge, TILE, width), kind),
            pltpu.VMEM((devices * max(first_turns, 1), BLOCK, width), kind),
            pltpu.VMEM((devices * (most - first_turns), BLOCK, width), kind),
            pltpu.VMEM((devices * max(first_turns, 1), BLOCK, width), kind),
            pltpu.SemaphoreType.DMA((2,)),
            pltpu.SemaphoreType.DMA,
            pltpu.SemaphoreType.DMA((2,)),
            pltpu.SemaphoreType.DMA((2,)),
            pltpu.SemaphoreType.DMA((2, devices)),
            pltpu.SemaphoreType.DMA((2, devices)),
        ],
        compiler_params=pltpu.CompilerParams(
            collective_id=0, has_side_effects=True, vmem_limit_bytes=57 * MIB
        ),
        name="exchange",
    )(picks, row_offsets, embed_rows.reshape(-1, TILE, width), head_rows.reshape(-1, TILE, width))


def finish(where, incoming, probe, n_data, n_tensor):
    columns, sketch_width = probe.shape
    kind = incoming.dtype
    slots = incoming.shape[0] // n_data
    most = slots // n_tensor
    buffers = 3
    smem = pl.BlockSpec(memory_space=pltpu.SMEM)
    vmem = pl.BlockSpec(memory_space=pltpu.VMEM)
    hbm = pl.BlockSpec(memory_space=pltpu.HBM)
    return pl.pallas_call(
        functools.partial(finish_kernel, n_data, n_tensor),
        in_specs=[smem, hbm, vmem],
        out_specs=[hbm, hbm],
        out_shape=[
            jax.ShapeDtypeStruct((slots, BLOCK, columns), kind),
            jax.ShapeDtypeStruct((slots, BLOCK, sketch_width), jnp.float32),
        ],
        scratch_shapes=[
            pltpu.SMEM((slots,), jnp.int32),
            pltpu.VMEM((n_tensor, most, BLOCK, columns), kind),
            pltpu.VMEM((buffers, most, BLOCK, sketch_width), jnp.float32),
            pltpu.SemaphoreType.DMA((n_tensor, n_data)),
            pltpu.SemaphoreType.DMA((n_tensor, most)),
            pltpu.SemaphoreType.DMA((buffers, most)),
        ],
        compiler_params=pltpu.CompilerParams(vmem_limit_bytes=57 * MIB),
        name="finish",
    )(where, incoming, probe)


def patch(where, fresh, probe, stored, sketch, n_data, n_tensor, first_turns):
    smem = pl.BlockSpec(memory_space=pltpu.SMEM)
    vmem = pl.BlockSpec(memory_space=pltpu.VMEM)
    hbm = pl.BlockSpec(memory_space=pltpu.HBM)
    return pl.pallas_call(
        functools.partial(patch_kernel, n_data, n_tensor, first_turns),
        in_specs=[smem, vmem, vmem, hbm, hbm],
        out_specs=[hbm, hbm],
        out_shape=[
            jax.ShapeDtypeStruct(stored.shape, stored.dtype),
            jax.ShapeDtypeStruct(sketch.shape, sketch.dtype),
        ],
        scratch_shapes=[
            pltpu.VMEM(stored.shape[1:], stored.dtype),
            pltpu.VMEM(sketch.shape[1:], sketch.dtype),
            pltpu.SemaphoreType.DMA((2,)),
        ],
        input_output_aliases={3: 0, 4: 1},
        compiler_params=pltpu.CompilerParams(vmem_limit_bytes=32 * MIB),
        name="patch",
    )(where, fresh, probe, stored, sketch)


def shards(embed_rows, head_rows, row_offsets, slot_table, probe):
    n_data, n_tensor = lax.axis_size("dp"), lax.axis_size("tensor")
    devices = n_data * n_tensor
    per_rank = slot_table.shape[0] // (2 * n_tensor)
    slots = slot_table.shape[0] // devices
    most = slots // n_tensor
    first_turns = most // 4
    picks, where, late = plan(row_offsets, slot_table.reshape(-1, LANES), n_tensor, per_rank, slots, first_turns)
    incoming, again = exchange(
        picks, row_offsets, embed_rows, head_rows, n_data, n_tensor, per_rank, most, first_turns
    )

    stored, sketch = finish(where, incoming, probe, n_data, n_tensor)
    if not first_turns:
        return stored, sketch

    def kept(where, again, probe, stored, sketch):
        return stored, sketch

    def resent(where, again, probe, stored, sketch):
        fresh = lax.all_to_all(again, AXES, split_axis=0, concat_axis=0, tiled=True)
        return tuple(patch(where, fresh, probe, stored, sketch, n_data, n_tensor, first_turns))

    return lax.cond(late[0, 0] == 0, kept, resent, where, again, probe, stored, sketch)


def solution(mesh):
    return jax.shard_map(
        shards,
        mesh=mesh,
        in_specs=(P("tensor", "dp"), P("tensor", "dp"), P(), P(), P()),
        out_specs=(P(AXES, None, None), P(AXES, None, None)),
        check_vma=False,
    )
```

```python
import functools

import jax
import jax.numpy as jnp
from jax import lax
from jax.experimental import pallas as pl
from jax.experimental.pallas import tpu as pltpu
from jax.sharding import PartitionSpec as P

MESH = pl.DeviceIdType.MESH
AXES = ("dp", "tensor")
BLOCK = 128
TILE = 16
WINDOW = 256
LANES = 128
MIB = 1 << 20


def tile_of(value):
    return lax.shift_right_arithmetic(value, 4)


def shallow_tiles(span):
    return 5 * (span // 4) // 8 // TILE


def tail_begin(offset, rank, span, height):
    return jnp.clip((rank + 1) * span - offset, 0, height - span // 4 - 1)


def selector(offset):
    row = lax.broadcasted_iota(jnp.int32, (BLOCK, WINDOW), 0)
    column = lax.broadcasted_iota(jnp.int32, (BLOCK, WINDOW), 1)
    return jnp.where(column - row == offset, 1.0, 0.0).astype(jnp.bfloat16)


def moved(offset, window):
    return jnp.dot(selector(offset), window, preferred_element_type=jnp.float32)


def plan_kernel(n_tensor, per_rank, slots, turns, offsets_ref, grid_ref, picks_ref, where_ref, *late_refs):
    me = lax.axis_index("tensor")
    span = per_rank * BLOCK
    grid = grid_ref[...]
    total = n_tensor * per_rank
    matrix = (grid >= total).astype(jnp.int32)
    within = grid - matrix * total
    source = lax.shift_right_logical(within, per_rank.bit_length() - 1)
    block = within - source * per_rank
    first = block * BLOCK
    shallow = shallow_tiles(span) * TILE
    level = jnp.zeros(grid.shape, jnp.int32)
    for m in range(2):
        for t in range(n_tensor):
            if t % 2 == 0:
                low = offsets_ref[m, t] - t * span
                touched = first < low
                need = jnp.minimum(first + BLOCK, low) + TILE
            else:
                high = offsets_ref[m, t + 1] - t * span
                touched = first + BLOCK > high
                need = first + BLOCK - high
            here = (source == t) & (matrix == m) & touched
            level = level + jnp.where(here, jnp.where(need > shallow, 2, 1), 0)
    lane = lax.broadcasted_iota(jnp.int32, grid.shape, 1)
    slot = lane % slots
    code = source * 4 + level
    floor = source * 4
    turn = jnp.zeros(grid.shape, jnp.int32)
    for k in range(1, slots):
        behind = pltpu.roll(code, k, 1)
        ahead = pltpu.roll(code, LANES - k, 1)
        turn = turn + jnp.where((slot >= k) & (behind >= floor) & (behind <= code), 1, 0)
        turn = turn + jnp.where((slot + k < slots) & (ahead >= floor) & (ahead < code), 1, 0)
    most = slots // n_tensor
    local = matrix * per_rank + block
    group_row = lax.broadcasted_iota(jnp.int32, (LANES, LANES), 0) // slots
    group_column = lax.broadcasted_iota(jnp.int32, (LANES, LANES), 1)
    picks = jnp.zeros(grid.shape, jnp.float32)
    for j in range(most):
        chosen = jnp.where((source == me) & (turn == j), local, 0).astype(jnp.float32)
        spread = jnp.where(group_column == group_row * most + j, 1.0, 0.0)
        picks = picks + jnp.dot(chosen, spread, preferred_element_type=jnp.float32)
    picks_ref[...] = picks.astype(jnp.int32)
    where_ref[...] = source * most + turn
    for phase, late_ref in enumerate(late_refs):
        ours = (turn >= sum(turns[:phase])) & (turn < sum(turns[: phase + 1]))
        wrong = jnp.where(ours & (level > phase), 1, 0)
        late_ref[...] = jnp.sum(jnp.sum(wrong, axis=1, keepdims=True), axis=0, keepdims=True)


def exchange_kernel(n_data, n_tensor, per_rank, turns, picks_ref, offsets_ref, embed_ref, head_ref,
                    incoming_ref, again_ref, again_second_ref, rows, trail, near, shallow, far, ready, second, rest, patched, patched_second,
                    load_sems, save_sem, keep_sems, edge_send, edge_recv, send_sems, recv_sems):
    data, rank = lax.axis_index("dp"), lax.axis_index("tensor")
    devices = n_data * n_tensor
    me = data * n_tensor + rank
    span = per_rank * BLOCK
    height = rows.shape[1] * TILE
    edge = trail.shape[1]
    most = incoming_ref.shape[0] // devices
    cut = shallow.shape[1]
    groups = LANES // (most * n_tensor)
    even = rank % 2 == 0
    near_rank = jnp.where(even, rank + 1, rank - 1)
    far_rank = jnp.where(even, (rank + n_tensor - 1) % n_tensor, (rank + 1) % n_tensor)
    left = (rank + n_tensor - 1) % n_tensor

    loads = [
        pltpu.make_async_copy(buffer, rows.at[m], load_sems.at[m])
        for m, buffer in enumerate((embed_ref, head_ref))
    ]
    for load in loads:
        load.start()

    def peer(k):
        return (data + k % n_data) % n_data, (rank + k // n_data) % n_tensor

    barrier = pltpu.get_barrier_semaphore()

    def greet(k, carry):
        d, t = peer(k)
        pl.semaphore_signal(barrier, inc=1, device_id=(d, t), device_id_type=MESH)
        return carry

    lax.fori_loop(1, devices, greet, 0)

    for load in loads:
        load.wait()

    def fill(i, carry):
        for m in range(2):
            trail[m, i] = rows[m, tile_of(tail_begin(offsets_ref[m, rank], rank, span, height)) + i]
        return carry

    lax.fori_loop(0, edge, fill, 0)
    pl.semaphore_wait(barrier, devices - 1)

    def edge_copy(source, target, which, t):
        return pltpu.make_async_remote_copy(
            src_ref=source, dst_ref=target, send_sem=edge_send.at[which], recv_sem=edge_recv.at[which],
            device_id=(data, t), device_id_type=MESH,
        )

    whole, upper, lower = pl.ds(0, edge), pl.ds(0, cut), pl.ds(cut, edge - cut)

    @pl.when(even)
    def _():
        edge_copy(trail, near, 0, near_rank).start()
        edge_copy(rows.at[:, upper], shallow, 1, far_rank).start()
        edge_copy(rows.at[:, lower], far.at[:, lower], 2, far_rank).start()

    @pl.when(jnp.logical_not(even))
    def _():
        edge_copy(rows.at[:, whole], near, 0, near_rank).start()
        edge_copy(trail.at[:, upper], shallow, 1, far_rank).start()
        edge_copy(trail.at[:, lower], far.at[:, lower], 2, far_rank).start()

    row = lax.broadcasted_iota(jnp.int32, (BLOCK, rows.shape[3]), 0)

    def window(buffer, m, start):
        base = jnp.clip(tile_of(start), 0, buffer.shape[1] - WINDOW // TILE)
        tiles = [buffer[m, base + i] for i in range(WINDOW // TILE)]
        return jnp.concatenate(tiles, axis=0), start - base * TILE

    def gathered(dest, j, beyond):
        number = picks_ref[dest // groups, dest % groups * most + j]
        m = (number >= per_rank).astype(jnp.int32)
        first = (number - m * per_rank) * BLOCK
        low = jnp.where(m == 0, offsets_ref[0, rank], offsets_ref[1, rank]) - rank * span - first
        high = jnp.where(m == 0, offsets_ref[0, rank + 1], offsets_ref[1, rank + 1]) - rank * span - first
        left_begin = tail_begin(jnp.where(m == 0, offsets_ref[0, left], offsets_ref[1, left]), left, span, height)
        own, own_offset = window(rows, m, -low)
        from_left = first + left_begin - tile_of(left_begin) * TILE
        from_right = -high
        piece, offset = window(near, m, jnp.where(even, from_right, from_left))
        if beyond is not None:
            use_far = jnp.where(even, low > 0, high < BLOCK)
            other, other_offset = window(beyond, m, jnp.where(even, from_left, from_right))
            piece = jnp.where(use_far, other, piece)
            offset = jnp.where(use_far, other_offset, offset)
        kept = moved(own_offset, own)
        patch = moved(offset, piece)
        return jnp.where((row >= low) & (row < high), kept, patch).astype(rows.dtype)

    def send(phase, staged, count, base, d, t):
        to = d * n_tensor + t
        return pltpu.make_async_remote_copy(
            src_ref=staged.at[pl.ds(to * count, count)],
            dst_ref=incoming_ref.at[pl.ds(me * most + base, count)],
            send_sem=send_sems.at[phase, to], recv_sem=recv_sems.at[phase, me],
            device_id=(d, t), device_id_type=MESH,
        )

    def keep(phase, staged, count, base):
        return pltpu.make_async_copy(
            staged.at[pl.ds(me * count, count)], incoming_ref.at[pl.ds(me * most + base, count)], keep_sems.at[phase]
        )

    edge_copies = [
        edge_copy(trail, near, 0, near_rank),
        edge_copy(trail.at[:, upper], shallow, 1, far_rank),
        edge_copy(trail.at[:, lower], far.at[:, lower], 2, far_rank),
    ]

    def phase_of(phase, staged, count, base, beyond):
        for j in range(count):
            staged[me * count + j] = gathered(me, base + j, beyond)

        def one(k, carry):
            d, t = peer(k)
            to = d * n_tensor + t
            for j in range(count):
                staged[to * count + j] = gathered(to, base + j, beyond)

            @pl.when(k > 1)
            def _():
                send(phase, staged, count, base, *peer(k - 1)).start()

            return carry

        lax.fori_loop(1, devices, one, 0)
        send(phase, staged, count, base, *peer(devices - 1)).start()
        keep(phase, staged, count, base).start()

    phases = [
        (phase, staged, count, sum(turns[:phase]), beyond)
        for phase, (staged, count, beyond) in enumerate(zip((ready, second, rest), turns, (None, shallow, far)))
        if count
    ]

    def join(i, carry):
        for m in range(2):
            far[m, i] = shallow[m, i]
        return carry

    for phase in range(3):
        edge_copies[phase].wait_recv()
        if phase == 2:
            lax.fori_loop(0, cut, join, 0)
        for entry in phases:
            if entry[0] == phase:
                phase_of(*entry)

    for entry, fixed, again in zip(phases, (patched, patched_second), (again_ref, again_second_ref)):
        phase, _, count, base, _ = entry
        if phase < 2:
            def redo(to, carry, fixed=fixed, count=count, base=base):
                for j in range(count):
                    fixed[to * count + j] = gathered(to, base + j, far)
                return carry

            lax.fori_loop(0, devices, redo, 0)
            save = pltpu.make_async_copy(fixed, again, save_sem)
            save.start()
            save.wait()

    for copy in edge_copies:
        copy.wait_send()

    def finish_phase(phase, staged, count, base):
        def drain(k, carry):
            d, t = peer(k)
            send(phase, staged, count, base, d, t).wait_send()
            pltpu.make_async_remote_copy(
                src_ref=staged.at[pl.ds(me * count, count)],
                dst_ref=incoming_ref.at[pl.ds((d * n_tensor + t) * most + base, count)],
                send_sem=send_sems.at[phase, me], recv_sem=recv_sems.at[phase, d * n_tensor + t],
                device_id=(d, t), device_id_type=MESH,
            ).wait_recv()
            return carry

        lax.fori_loop(1, devices, drain, 0)
        keep(phase, staged, count, base).wait()

    for entry in phases:
        finish_phase(*entry[:4])


def finish_kernel(n_data, n_tensor, where_ref, incoming_ref, probe_ref, stored_ref, sketch_ref,
                  slot_of, stored, sketch, load_sems, stored_sems, sketch_sems):
    width = incoming_ref.shape[2]
    slots = stored_ref.shape[0]
    most, groups = slots // n_tensor, LANES // slots
    buffers = sketch.shape[0]
    me = lax.axis_index("dp") * n_tensor + lax.axis_index("tensor")
    for t in range(n_tensor):
        for d in range(n_data):
            pltpu.make_async_copy(
                incoming_ref.at[pl.ds((d * n_tensor + t) * most, most)],
                stored.at[t, :, :, pl.ds(d * width, width)],
                load_sems.at[t, d],
            ).start()
    for s in range(slots):
        slot_of[where_ref[me // groups, me % groups * slots + s]] = s

    def writes(t):
        b = t % buffers
        copies = []
        for r in range(most):
            slot = slot_of[t * most + r]
            copies.append(pltpu.make_async_copy(sketch.at[b, r], sketch_ref.at[slot], sketch_sems.at[b, r]))
            copies.append(pltpu.make_async_copy(stored.at[t, r], stored_ref.at[slot], stored_sems.at[t, r]))
        return copies

    for t in range(n_tensor):
        b = t % buffers
        for d in range(n_data):
            pltpu.make_async_copy(
                incoming_ref.at[pl.ds((d * n_tensor + t) * most, most)],
                stored.at[t, :, :, pl.ds(d * width, width)],
                load_sems.at[t, d],
            ).wait()
        if t >= buffers:
            for write in writes(t - buffers):
                write.wait()
        rows = stored[t].reshape(most * BLOCK, n_data * width)
        product = jnp.dot(rows, probe_ref[...], preferred_element_type=jnp.float32)
        sketch[b] = product.reshape(sketch.shape[1:])
        for write in writes(t):
            write.start()
    for t in range(max(n_tensor - buffers, 0), n_tensor):
        for write in writes(t):
            write.wait()


def patch_kernel(n_data, n_tensor, begin, count, where_ref, fresh_ref, probe_ref, old_stored_ref, old_sketch_ref,
                 stored_ref, sketch_ref, stored, sketch, sems):
    width = fresh_ref.shape[2]
    slots = stored_ref.shape[0]
    most, groups = slots // n_tensor, LANES // slots
    me = lax.axis_index("dp") * n_tensor + lax.axis_index("tensor")

    def one(slot, carry):
        base = where_ref[me // groups, me % groups * slots + slot]
        turn = base % most

        @pl.when((turn >= begin) & (turn < begin + count))
        def _():
            for d in range(n_data):
                held = (base // most + d * n_tensor) * count + turn - begin
                stored[:, d * width : (d + 1) * width] = fresh_ref[held]
            sketch[...] = jnp.dot(stored[...], probe_ref[...], preferred_element_type=jnp.float32)
            writes = (
                pltpu.make_async_copy(stored, stored_ref.at[slot], sems.at[0]),
                pltpu.make_async_copy(sketch, sketch_ref.at[slot], sems.at[1]),
            )
            for write in writes:
                write.start()
            for write in writes:
                write.wait()

        return carry

    lax.fori_loop(0, slots, one, 0)


def plan(row_offsets, grid, n_tensor, per_rank, slots, turns):
    vmem = pl.BlockSpec(memory_space=pltpu.VMEM)
    return pl.pallas_call(
        functools.partial(plan_kernel, n_tensor, per_rank, slots, turns),
        in_specs=[pl.BlockSpec(memory_space=pltpu.SMEM), vmem],
        out_specs=[vmem, vmem, vmem, vmem],
        out_shape=[
            jax.ShapeDtypeStruct(grid.shape, jnp.int32),
            jax.ShapeDtypeStruct(grid.shape, jnp.int32),
            jax.ShapeDtypeStruct((1, 1), jnp.int32),
            jax.ShapeDtypeStruct((1, 1), jnp.int32),
        ],
        name="plan",
    )(row_offsets, grid)


def exchange(picks, row_offsets, embed_rows, head_rows, n_data, n_tensor, per_rank, most, turns):
    height, width = embed_rows.shape
    kind = embed_rows.dtype
    devices = n_data * n_tensor
    edge = per_rank * BLOCK // 4 // TILE + 1
    smem = pl.BlockSpec(memory_space=pltpu.SMEM)
    hbm = pl.BlockSpec(memory_space=pltpu.HBM)

    def blocks(count):
        return pltpu.VMEM((devices * max(count, 1), BLOCK, width), kind)

    def tiles(count):
        return pltpu.VMEM((2, count, TILE, width), kind)

    return pl.pallas_call(
        functools.partial(exchange_kernel, n_data, n_tensor, per_rank, turns),
        in_specs=[smem, smem, hbm, hbm],
        out_specs=[hbm, hbm, hbm],
        out_shape=[
            jax.ShapeDtypeStruct((devices * most, BLOCK, width), kind),
            jax.ShapeDtypeStruct((devices * max(turns[0], 1), BLOCK, width), kind),
            jax.ShapeDtypeStruct((devices * max(turns[1], 1), BLOCK, width), kind),
        ],
        scratch_shapes=[
            tiles(height // TILE),
            tiles(edge),
            tiles(edge),
            tiles(shallow_tiles(per_rank * BLOCK)),
            tiles(edge),
            blocks(turns[0]),
            blocks(turns[1]),
            blocks(turns[2]),
            blocks(turns[0]),
            blocks(turns[1]),
            pltpu.SemaphoreType.DMA((2,)),
            pltpu.SemaphoreType.DMA,
            pltpu.SemaphoreType.DMA((3,)),
            pltpu.SemaphoreType.DMA((3,)),
            pltpu.SemaphoreType.DMA((3,)),
            pltpu.SemaphoreType.DMA((3, devices)),
            pltpu.SemaphoreType.DMA((3, devices)),
        ],
        compiler_params=pltpu.CompilerParams(
            collective_id=0, has_side_effects=True, vmem_limit_bytes=57 * MIB
        ),
        name="exchange",
    )(picks, row_offsets, embed_rows.reshape(-1, TILE, width), head_rows.reshape(-1, TILE, width))


def finish(where, incoming, probe, n_data, n_tensor):
    columns, sketch_width = probe.shape
    kind = incoming.dtype
    slots = incoming.shape[0] // n_data
    most = slots // n_tensor
    buffers = 3
    smem = pl.BlockSpec(memory_space=pltpu.SMEM)
    vmem = pl.BlockSpec(memory_space=pltpu.VMEM)
    hbm = pl.BlockSpec(memory_space=pltpu.HBM)
    return pl.pallas_call(
        functools.partial(finish_kernel, n_data, n_tensor),
        in_specs=[smem, hbm, vmem],
        out_specs=[hbm, hbm],
        out_shape=[
            jax.ShapeDtypeStruct((slots, BLOCK, columns), kind),
            jax.ShapeDtypeStruct((slots, BLOCK, sketch_width), jnp.float32),
        ],
        scratch_shapes=[
            pltpu.SMEM((slots,), jnp.int32),
            pltpu.VMEM((n_tensor, most, BLOCK, columns), kind),
            pltpu.VMEM((buffers, most, BLOCK, sketch_width), jnp.float32),
            pltpu.SemaphoreType.DMA((n_tensor, n_data)),
            pltpu.SemaphoreType.DMA((n_tensor, most)),
            pltpu.SemaphoreType.DMA((buffers, most)),
        ],
        compiler_params=pltpu.CompilerParams(vmem_limit_bytes=57 * MIB),
        name="finish",
    )(where, incoming, probe)


def patch(where, fresh, probe, stored, sketch, n_data, n_tensor, begin, count):
    smem = pl.BlockSpec(memory_space=pltpu.SMEM)
    vmem = pl.BlockSpec(memory_space=pltpu.VMEM)
    hbm = pl.BlockSpec(memory_space=pltpu.HBM)
    return pl.pallas_call(
        functools.partial(patch_kernel, n_data, n_tensor, begin, count),
        in_specs=[smem, vmem, vmem, hbm, hbm],
        out_specs=[hbm, hbm],
        out_shape=[
            jax.ShapeDtypeStruct(stored.shape, stored.dtype),
            jax.ShapeDtypeStruct(sketch.shape, sketch.dtype),
        ],
        scratch_shapes=[
            pltpu.VMEM(stored.shape[1:], stored.dtype),
            pltpu.VMEM(sketch.shape[1:], sketch.dtype),
            pltpu.SemaphoreType.DMA((2,)),
        ],
        input_output_aliases={3: 0, 4: 1},
        compiler_params=pltpu.CompilerParams(vmem_limit_bytes=32 * MIB),
        name="patch",
    )(where, fresh, probe, stored, sketch)


def shards(embed_rows, head_rows, row_offsets, slot_table, probe):
    n_data, n_tensor = lax.axis_size("dp"), lax.axis_size("tensor")
    devices = n_data * n_tensor
    per_rank = slot_table.shape[0] // (2 * n_tensor)
    slots = slot_table.shape[0] // devices
    most = slots // n_tensor
    turns = (most // 4, most // 4, most - 2 * (most // 4))
    picks, where, *late = plan(row_offsets, slot_table.reshape(-1, LANES), n_tensor, per_rank, slots, turns)
    incoming, *again = exchange(
        picks, row_offsets, embed_rows, head_rows, n_data, n_tensor, per_rank, most, turns
    )
    result = tuple(finish(where, incoming, probe, n_data, n_tensor))

    def kept(where, again, probe, result):
        return result

    def resent(begin, count, where, again, probe, result):
        fresh = lax.all_to_all(again, AXES, split_axis=0, concat_axis=0, tiled=True)
        return tuple(patch(where, fresh, probe, *result, n_data, n_tensor, begin, count))

    for phase in range(2):
        if turns[phase]:
            other = functools.partial(resent, sum(turns[:phase]), turns[phase])
            result = lax.cond(late[phase][0, 0] == 0, kept, other, where, again[phase], probe, result)
    return result


def solution(mesh):
    return jax.shard_map(
        shards,
        mesh=mesh,
        in_specs=(P("tensor", "dp"), P("tensor", "dp"), P(), P(), P()),
        out_specs=(P(AXES, None, None), P(AXES, None, None)),
        check_vma=False,
    )
```

```python
import functools

import jax
import jax.numpy as jnp
from jax import lax
from jax.experimental import pallas as pl
from jax.experimental.pallas import tpu as pltpu
from jax.sharding import PartitionSpec as P

MESH = pl.DeviceIdType.MESH
AXES = ("dp", "tensor")
BLOCK = 128
TILE = 16
WINDOW = 256
LANES = 128
MIB = 1 << 20


def tile_of(value):
    return lax.shift_right_arithmetic(value, 4)


def shallow_tiles(span):
    return 5 * (span // 4) // 8 // TILE


def tail_begin(offset, rank, span, height):
    return jnp.clip((rank + 1) * span - offset, 0, height - span // 4 - 1)


def selector(offset):
    row = lax.broadcasted_iota(jnp.int32, (BLOCK, WINDOW), 0)
    column = lax.broadcasted_iota(jnp.int32, (BLOCK, WINDOW), 1)
    return jnp.where(column - row == offset, 1.0, 0.0).astype(jnp.bfloat16)


def moved(offset, window):
    return jnp.dot(selector(offset), window, preferred_element_type=jnp.float32)


def plan(me, n_tensor, per_rank, slots, turns, offsets_ref, grid):
    span = per_rank * BLOCK
    total = n_tensor * per_rank
    matrix = (grid >= total).astype(jnp.int32)
    within = grid - matrix * total
    source = lax.shift_right_logical(within, per_rank.bit_length() - 1)
    block = within - source * per_rank
    first = block * BLOCK
    shallow = shallow_tiles(span) * TILE
    level = jnp.zeros(grid.shape, jnp.int32)
    for m in range(2):
        for t in range(n_tensor):
            if t % 2 == 0:
                low = offsets_ref[m, t] - t * span
                touched = first < low
                need = jnp.minimum(first + BLOCK, low) + TILE
            else:
                high = offsets_ref[m, t + 1] - t * span
                touched = first + BLOCK > high
                need = first + BLOCK - high
            here = (source == t) & (matrix == m) & touched
            level = level + jnp.where(here, jnp.where(need > shallow, 2, 1), 0)
    lane = lax.broadcasted_iota(jnp.int32, grid.shape, 1)
    slot = lane % slots
    code = source * 4 + level
    floor = source * 4
    turn = jnp.zeros(grid.shape, jnp.int32)
    for k in range(1, slots):
        behind = pltpu.roll(code, k, 1)
        ahead = pltpu.roll(code, LANES - k, 1)
        turn = turn + jnp.where((slot >= k) & (behind >= floor) & (behind <= code), 1, 0)
        turn = turn + jnp.where((slot + k < slots) & (ahead >= floor) & (ahead < code), 1, 0)
    most = slots // n_tensor
    local = matrix * per_rank + block
    group_row = lax.broadcasted_iota(jnp.int32, (LANES, LANES), 0) // slots
    group_column = lax.broadcasted_iota(jnp.int32, (LANES, LANES), 1)
    picks = jnp.zeros(grid.shape, jnp.float32)
    for j in range(most):
        chosen = jnp.where((source == me) & (turn == j), local, 0).astype(jnp.float32)
        spread = jnp.where(group_column == group_row * most + j, 1.0, 0.0)
        picks = picks + jnp.dot(chosen, spread, preferred_element_type=jnp.float32)
    late = jnp.zeros(grid.shape, jnp.int32)
    for phase in range(2):
        ours = (turn >= sum(turns[:phase])) & (turn < sum(turns[: phase + 1]))
        wrong = jnp.where(ours & (level > phase), 1, 0)
        wrong = jnp.sum(jnp.sum(wrong, axis=1, keepdims=True), axis=0, keepdims=True)
        late = jnp.where(lane == phase, wrong, late)
    return picks.astype(jnp.int32), source * most + turn, late


def exchange_kernel(n_data, n_tensor, per_rank, turns, offsets_ref, table_ref, embed_ref, head_ref,
                    incoming_ref, again_ref, again_second_ref, where_ref, late_ref,
                    table, notes, picks, rows, trail, near, shallow, far, ready, second, rest, patched, patched_second,
                    load_sems, note_sems, save_sem, keep_sems, edge_send, edge_recv, send_sems, recv_sems):
    data, rank = lax.axis_index("dp"), lax.axis_index("tensor")
    devices = n_data * n_tensor
    me = data * n_tensor + rank
    span = per_rank * BLOCK
    height = rows.shape[1] * TILE
    edge = trail.shape[1]
    most = incoming_ref.shape[0] // devices
    cut = shallow.shape[1]
    groups = LANES // (most * n_tensor)
    even = rank % 2 == 0
    near_rank = jnp.where(even, rank + 1, rank - 1)
    far_rank = jnp.where(even, (rank + n_tensor - 1) % n_tensor, (rank + 1) % n_tensor)
    left = (rank + n_tensor - 1) % n_tensor

    loads = [
        pltpu.make_async_copy(buffer, rows.at[m], load_sems.at[m])
        for m, buffer in enumerate((embed_ref, head_ref))
    ]
    read = pltpu.make_async_copy(table_ref, table, note_sems.at[0])
    read.start()
    for load in loads:
        load.start()

    def peer(k):
        return (data + k % n_data) % n_data, (rank + k // n_data) % n_tensor

    barrier = pltpu.get_barrier_semaphore()

    def greet(k, carry):
        d, t = peer(k)
        pl.semaphore_signal(barrier, inc=1, device_id=(d, t), device_id_type=MESH)
        return carry

    lax.fori_loop(1, devices, greet, 0)

    read.wait()
    found = plan(rank, n_tensor, per_rank, most * n_tensor, turns, offsets_ref, table[...])
    for i in range(3):
        notes[i] = found[i]
    for load in loads:
        load.wait()

    def fill(i, carry):
        for m in range(2):
            trail[m, i] = rows[m, tile_of(tail_begin(offsets_ref[m, rank], rank, span, height)) + i]
        return carry

    lax.fori_loop(0, edge, fill, 0)
    note = pltpu.make_async_copy(notes, picks, note_sems.at[0])
    note.start()
    pass_on = pltpu.make_async_copy(notes.at[1], where_ref, note_sems.at[1])
    pass_on.start()
    pl.semaphore_wait(barrier, devices - 1)

    def edge_copy(source, target, which, t):
        return pltpu.make_async_remote_copy(
            src_ref=source, dst_ref=target, send_sem=edge_send.at[which], recv_sem=edge_recv.at[which],
            device_id=(data, t), device_id_type=MESH,
        )

    whole, upper, lower = pl.ds(0, edge), pl.ds(0, cut), pl.ds(cut, edge - cut)

    @pl.when(even)
    def _():
        edge_copy(trail, near, 0, near_rank).start()
        edge_copy(rows.at[:, upper], shallow, 1, far_rank).start()
        edge_copy(rows.at[:, lower], far.at[:, lower], 2, far_rank).start()

    @pl.when(jnp.logical_not(even))
    def _():
        edge_copy(rows.at[:, whole], near, 0, near_rank).start()
        edge_copy(trail.at[:, upper], shallow, 1, far_rank).start()
        edge_copy(trail.at[:, lower], far.at[:, lower], 2, far_rank).start()

    row = lax.broadcasted_iota(jnp.int32, (BLOCK, rows.shape[3]), 0)

    def window(buffer, m, start):
        base = jnp.clip(tile_of(start), 0, buffer.shape[1] - WINDOW // TILE)
        tiles = [buffer[m, base + i] for i in range(WINDOW // TILE)]
        return jnp.concatenate(tiles, axis=0), start - base * TILE

    def gathered(dest, j, beyond):
        number = picks[0, dest // groups, dest % groups * most + j]
        m = (number >= per_rank).astype(jnp.int32)
        first = (number - m * per_rank) * BLOCK
        low = jnp.where(m == 0, offsets_ref[0, rank], offsets_ref[1, rank]) - rank * span - first
        high = jnp.where(m == 0, offsets_ref[0, rank + 1], offsets_ref[1, rank + 1]) - rank * span - first
        left_begin = tail_begin(jnp.where(m == 0, offsets_ref[0, left], offsets_ref[1, left]), left, span, height)
        own, own_offset = window(rows, m, -low)
        from_left = first + left_begin - tile_of(left_begin) * TILE
        from_right = -high
        piece, offset = window(near, m, jnp.where(even, from_right, from_left))
        if beyond is not None:
            use_far = jnp.where(even, low > 0, high < BLOCK)
            other, other_offset = window(beyond, m, jnp.where(even, from_left, from_right))
            piece = jnp.where(use_far, other, piece)
            offset = jnp.where(use_far, other_offset, offset)
        kept = moved(own_offset, own)
        patch = moved(offset, piece)
        return jnp.where((row >= low) & (row < high), kept, patch).astype(rows.dtype)

    def send(phase, staged, count, base, d, t):
        to = d * n_tensor + t
        return pltpu.make_async_remote_copy(
            src_ref=staged.at[pl.ds(to * count, count)],
            dst_ref=incoming_ref.at[pl.ds(me * most + base, count)],
            send_sem=send_sems.at[phase, to], recv_sem=recv_sems.at[phase, me],
            device_id=(d, t), device_id_type=MESH,
        )

    def keep(phase, staged, count, base):
        return pltpu.make_async_copy(
            staged.at[pl.ds(me * count, count)], incoming_ref.at[pl.ds(me * most + base, count)], keep_sems.at[phase]
        )

    edge_copies = [
        edge_copy(trail, near, 0, near_rank),
        edge_copy(trail.at[:, upper], shallow, 1, far_rank),
        edge_copy(trail.at[:, lower], far.at[:, lower], 2, far_rank),
    ]

    def phase_of(phase, staged, count, base, beyond):
        for j in range(count):
            staged[me * count + j] = gathered(me, base + j, beyond)

        def one(k, carry):
            d, t = peer(k)
            to = d * n_tensor + t
            for j in range(count):
                staged[to * count + j] = gathered(to, base + j, beyond)

            @pl.when(k > 1)
            def _():
                send(phase, staged, count, base, *peer(k - 1)).start()

            return carry

        lax.fori_loop(1, devices, one, 0)
        send(phase, staged, count, base, *peer(devices - 1)).start()
        keep(phase, staged, count, base).start()

    phases = [
        (phase, staged, count, sum(turns[:phase]), beyond)
        for phase, (staged, count, beyond) in enumerate(zip((ready, second, rest), turns, (None, shallow, far)))
        if count
    ]

    def join(i, carry):
        for m in range(2):
            far[m, i] = shallow[m, i]
        return carry

    note.wait()
    pass_on.wait()
    late_ref[0, 0] = jnp.minimum(picks[2, 0, 0], 1) + 2 * jnp.minimum(picks[2, 0, 1], 1)
    for phase in range(3):
        edge_copies[phase].wait_recv()
        if phase == 2:
            lax.fori_loop(0, cut, join, 0)
        for entry in phases:
            if entry[0] == phase:
                phase_of(*entry)

    for entry, fixed, again in zip(phases, (patched, patched_second), (again_ref, again_second_ref)):
        phase, _, count, base, _ = entry
        if phase < 2:
            def redo(to, carry, fixed=fixed, count=count, base=base):
                for j in range(count):
                    fixed[to * count + j] = gathered(to, base + j, far)
                return carry

            lax.fori_loop(0, devices, redo, 0)
            save = pltpu.make_async_copy(fixed, again, save_sem)
            save.start()
            save.wait()

    for copy in edge_copies:
        copy.wait_send()

    def finish_phase(phase, staged, count, base):
        def drain(k, carry):
            d, t = peer(k)
            send(phase, staged, count, base, d, t).wait_send()
            pltpu.make_async_remote_copy(
                src_ref=staged.at[pl.ds(me * count, count)],
                dst_ref=incoming_ref.at[pl.ds((d * n_tensor + t) * most + base, count)],
                send_sem=send_sems.at[phase, me], recv_sem=recv_sems.at[phase, d * n_tensor + t],
                device_id=(d, t), device_id_type=MESH,
            ).wait_recv()
            return carry

        lax.fori_loop(1, devices, drain, 0)
        keep(phase, staged, count, base).wait()

    for entry in phases:
        finish_phase(*entry[:4])


def finish_kernel(n_data, n_tensor, where_ref, incoming_ref, probe_ref, stored_ref, sketch_ref,
                  slot_of, stored, sketch, load_sems, stored_sems, sketch_sems):
    width = incoming_ref.shape[2]
    slots = stored_ref.shape[0]
    most, groups = slots // n_tensor, LANES // slots
    buffers = sketch.shape[0]
    me = lax.axis_index("dp") * n_tensor + lax.axis_index("tensor")
    for t in range(n_tensor):
        for d in range(n_data):
            pltpu.make_async_copy(
                incoming_ref.at[pl.ds((d * n_tensor + t) * most, most)],
                stored.at[t, :, :, pl.ds(d * width, width)],
                load_sems.at[t, d],
            ).start()
    for s in range(slots):
        slot_of[where_ref[me // groups, me % groups * slots + s]] = s

    def writes(t):
        b = t % buffers
        copies = []
        for r in range(most):
            slot = slot_of[t * most + r]
            copies.append(pltpu.make_async_copy(sketch.at[b, r], sketch_ref.at[slot], sketch_sems.at[b, r]))
            copies.append(pltpu.make_async_copy(stored.at[t, r], stored_ref.at[slot], stored_sems.at[t, r]))
        return copies

    for t in range(n_tensor):
        b = t % buffers
        for d in range(n_data):
            pltpu.make_async_copy(
                incoming_ref.at[pl.ds((d * n_tensor + t) * most, most)],
                stored.at[t, :, :, pl.ds(d * width, width)],
                load_sems.at[t, d],
            ).wait()
        if t >= buffers:
            for write in writes(t - buffers):
                write.wait()
        rows = stored[t].reshape(most * BLOCK, n_data * width)
        product = jnp.dot(rows, probe_ref[...], preferred_element_type=jnp.float32)
        sketch[b] = product.reshape(sketch.shape[1:])
        for write in writes(t):
            write.start()
    for t in range(max(n_tensor - buffers, 0), n_tensor):
        for write in writes(t):
            write.wait()


def patch_kernel(n_data, n_tensor, begin, count, where_ref, fresh_ref, probe_ref, old_stored_ref, old_sketch_ref,
                 stored_ref, sketch_ref, stored, sketch, sems):
    width = fresh_ref.shape[2]
    slots = stored_ref.shape[0]
    most, groups = slots // n_tensor, LANES // slots
    me = lax.axis_index("dp") * n_tensor + lax.axis_index("tensor")

    def one(slot, carry):
        base = where_ref[me // groups, me % groups * slots + slot]
        turn = base % most

        @pl.when((turn >= begin) & (turn < begin + count))
        def _():
            for d in range(n_data):
                held = (base // most + d * n_tensor) * count + turn - begin
                stored[:, d * width : (d + 1) * width] = fresh_ref[held]
            sketch[...] = jnp.dot(stored[...], probe_ref[...], preferred_element_type=jnp.float32)
            writes = (
                pltpu.make_async_copy(stored, stored_ref.at[slot], sems.at[0]),
                pltpu.make_async_copy(sketch, sketch_ref.at[slot], sems.at[1]),
            )
            for write in writes:
                write.start()
            for write in writes:
                write.wait()

        return carry

    lax.fori_loop(0, slots, one, 0)


def exchange(row_offsets, table, embed_rows, head_rows, n_data, n_tensor, per_rank, most, turns):
    height, width = embed_rows.shape
    kind = embed_rows.dtype
    devices = n_data * n_tensor
    edge = per_rank * BLOCK // 4 // TILE + 1
    smem = pl.BlockSpec(memory_space=pltpu.SMEM)
    hbm = pl.BlockSpec(memory_space=pltpu.HBM)

    def blocks(count):
        return pltpu.VMEM((devices * max(count, 1), BLOCK, width), kind)

    def tiles(count):
        return pltpu.VMEM((2, count, TILE, width), kind)

    return pl.pallas_call(
        functools.partial(exchange_kernel, n_data, n_tensor, per_rank, turns),
        in_specs=[smem, hbm, hbm, hbm],
        out_specs=[hbm, hbm, hbm, hbm, smem],
        out_shape=[
            jax.ShapeDtypeStruct((devices * most, BLOCK, width), kind),
            jax.ShapeDtypeStruct((devices * max(turns[0], 1), BLOCK, width), kind),
            jax.ShapeDtypeStruct((devices * max(turns[1], 1), BLOCK, width), kind),
            jax.ShapeDtypeStruct(table.shape, jnp.int32),
            jax.ShapeDtypeStruct((1, 1), jnp.int32),
        ],
        scratch_shapes=[
            pltpu.VMEM(table.shape, jnp.int32),
            pltpu.VMEM((3,) + table.shape, jnp.int32),
            pltpu.SMEM((3,) + table.shape, jnp.int32),
            tiles(height // TILE),
            tiles(edge),
            tiles(edge),
            tiles(shallow_tiles(per_rank * BLOCK)),
            tiles(edge),
            blocks(turns[0]),
            blocks(turns[1]),
            blocks(turns[2]),
            blocks(turns[0]),
            blocks(turns[1]),
            pltpu.SemaphoreType.DMA((2,)),
            pltpu.SemaphoreType.DMA((2,)),
            pltpu.SemaphoreType.DMA,
            pltpu.SemaphoreType.DMA((3,)),
            pltpu.SemaphoreType.DMA((3,)),
            pltpu.SemaphoreType.DMA((3,)),
            pltpu.SemaphoreType.DMA((3, devices)),
            pltpu.SemaphoreType.DMA((3, devices)),
        ],
        compiler_params=pltpu.CompilerParams(
            collective_id=0, has_side_effects=True, vmem_limit_bytes=57 * MIB
        ),
        name="exchange",
    )(row_offsets, table, embed_rows.reshape(-1, TILE, width), head_rows.reshape(-1, TILE, width))


def finish(where, incoming, probe, n_data, n_tensor):
    columns, sketch_width = probe.shape
    kind = incoming.dtype
    slots = incoming.shape[0] // n_data
    most = slots // n_tensor
    buffers = 3
    smem = pl.BlockSpec(memory_space=pltpu.SMEM)
    vmem = pl.BlockSpec(memory_space=pltpu.VMEM)
    hbm = pl.BlockSpec(memory_space=pltpu.HBM)
    return pl.pallas_call(
        functools.partial(finish_kernel, n_data, n_tensor),
        in_specs=[smem, hbm, vmem],
        out_specs=[hbm, hbm],
        out_shape=[
            jax.ShapeDtypeStruct((slots, BLOCK, columns), kind),
            jax.ShapeDtypeStruct((slots, BLOCK, sketch_width), jnp.float32),
        ],
        scratch_shapes=[
            pltpu.SMEM((slots,), jnp.int32),
            pltpu.VMEM((n_tensor, most, BLOCK, columns), kind),
            pltpu.VMEM((buffers, most, BLOCK, sketch_width), jnp.float32),
            pltpu.SemaphoreType.DMA((n_tensor, n_data)),
            pltpu.SemaphoreType.DMA((n_tensor, most)),
            pltpu.SemaphoreType.DMA((buffers, most)),
        ],
        compiler_params=pltpu.CompilerParams(vmem_limit_bytes=57 * MIB),
        name="finish",
    )(where, incoming, probe)


def patch(where, fresh, probe, stored, sketch, n_data, n_tensor, begin, count):
    smem = pl.BlockSpec(memory_space=pltpu.SMEM)
    vmem = pl.BlockSpec(memory_space=pltpu.VMEM)
    hbm = pl.BlockSpec(memory_space=pltpu.HBM)
    return pl.pallas_call(
        functools.partial(patch_kernel, n_data, n_tensor, begin, count),
        in_specs=[smem, vmem, vmem, hbm, hbm],
        out_specs=[hbm, hbm],
        out_shape=[
            jax.ShapeDtypeStruct(stored.shape, stored.dtype),
            jax.ShapeDtypeStruct(sketch.shape, sketch.dtype),
        ],
        scratch_shapes=[
            pltpu.VMEM(stored.shape[1:], stored.dtype),
            pltpu.VMEM(sketch.shape[1:], sketch.dtype),
            pltpu.SemaphoreType.DMA((2,)),
        ],
        input_output_aliases={3: 0, 4: 1},
        compiler_params=pltpu.CompilerParams(vmem_limit_bytes=32 * MIB),
        name="patch",
    )(where, fresh, probe, stored, sketch)


def shards(embed_rows, head_rows, row_offsets, slot_table, probe):
    n_data, n_tensor = lax.axis_size("dp"), lax.axis_size("tensor")
    devices = n_data * n_tensor
    per_rank = slot_table.shape[0] // (2 * n_tensor)
    slots = slot_table.shape[0] // devices
    most = slots // n_tensor
    turns = (most // 4, most // 4, most - 2 * (most // 4))
    incoming, first, second, where, late = exchange(
        row_offsets, slot_table.reshape(-1, LANES), embed_rows, head_rows, n_data, n_tensor, per_rank, most, turns
    )
    again = (first, second)
    result = tuple(finish(where, incoming, probe, n_data, n_tensor))

    def kept(where, again, probe, result):
        return result

    def resent(begin, count, phase, where, again, probe, result):
        fresh = lax.all_to_all(again[phase], AXES, split_axis=0, concat_axis=0, tiled=True)
        return tuple(patch(where, fresh, probe, *result, n_data, n_tensor, begin, count))

    def both(*args):
        return redone[1](*args[:-1], redone[0](*args))

    redone = [
        functools.partial(resent, sum(turns[:phase]), turns[phase], phase) for phase in range(2)
    ]
    if not turns[0]:
        return result
    return lax.switch(late[0, 0], [kept, *redone, both], where, again, probe, result)


def solution(mesh):
    return jax.shard_map(
        shards,
        mesh=mesh,
        in_specs=(P("tensor", "dp"), P("tensor", "dp"), P(), P(), P()),
        out_specs=(P(AXES, None, None), P(AXES, None, None)),
        check_vma=False,
    )
```

```python
import functools

import jax
import jax.numpy as jnp
from jax import lax
from jax.experimental import pallas as pl
from jax.experimental.pallas import tpu as pltpu
from jax.sharding import PartitionSpec as P

MESH = pl.DeviceIdType.MESH
AXES = ("dp", "tensor")
BLOCK = 128
TILE = 16
WINDOW = 256
LANES = 128
MIB = 1 << 20


def tile_of(value):
    return lax.shift_right_arithmetic(value, 4)


def shallow_tiles(span):
    return 5 * (span // 4) // 8 // TILE


def tail_begin(offset, rank, span, height):
    return jnp.clip((rank + 1) * span - offset, 0, height - span // 4 - 1)


def selector(offset):
    row = lax.broadcasted_iota(jnp.int32, (BLOCK, WINDOW), 0)
    column = lax.broadcasted_iota(jnp.int32, (BLOCK, WINDOW), 1)
    return jnp.where(column - row == offset, 1.0, 0.0).astype(jnp.bfloat16)


def moved(offset, window):
    return jnp.dot(selector(offset), window, preferred_element_type=jnp.float32)


def plan(me, n_tensor, per_rank, slots, turns, offsets_ref, grid):
    span = per_rank * BLOCK
    total = n_tensor * per_rank
    matrix = (grid >= total).astype(jnp.int32)
    within = grid - matrix * total
    source = lax.shift_right_logical(within, per_rank.bit_length() - 1)
    block = within - source * per_rank
    first = block * BLOCK
    shallow = shallow_tiles(span) * TILE
    level = jnp.zeros(grid.shape, jnp.int32)
    for m in range(2):
        for t in range(n_tensor):
            if t % 2 == 0:
                low = offsets_ref[m, t] - t * span
                touched = first < low
                need = jnp.minimum(first + BLOCK, low) + TILE
            else:
                high = offsets_ref[m, t + 1] - t * span
                touched = first + BLOCK > high
                need = first + BLOCK - high
            here = (source == t) & (matrix == m) & touched
            level = level + jnp.where(here, jnp.where(need > shallow, 2, 1), 0)
    lane = lax.broadcasted_iota(jnp.int32, grid.shape, 1)
    slot = lane % slots
    code = source * 4 + level
    floor = source * 4
    turn = jnp.zeros(grid.shape, jnp.int32)
    for k in range(1, slots):
        behind = pltpu.roll(code, k, 1)
        ahead = pltpu.roll(code, LANES - k, 1)
        turn = turn + jnp.where((slot >= k) & (behind >= floor) & (behind <= code), 1, 0)
        turn = turn + jnp.where((slot + k < slots) & (ahead >= floor) & (ahead < code), 1, 0)
    most = slots // n_tensor
    local = matrix * per_rank + block
    group_row = lax.broadcasted_iota(jnp.int32, (LANES, LANES), 0) // slots
    group_column = lax.broadcasted_iota(jnp.int32, (LANES, LANES), 1)
    picks = jnp.zeros(grid.shape, jnp.float32)
    for j in range(most):
        chosen = jnp.where((source == me) & (turn == j), local, 0).astype(jnp.float32)
        spread = jnp.where(group_column == group_row * most + j, 1.0, 0.0)
        picks = picks + jnp.dot(chosen, spread, preferred_element_type=jnp.float32)
    late = jnp.zeros(grid.shape, jnp.int32)
    for phase in range(2):
        ours = (turn >= sum(turns[:phase])) & (turn < sum(turns[: phase + 1]))
        wrong = jnp.where(ours & (level > phase), 1, 0)
        wrong = jnp.sum(jnp.sum(wrong, axis=1, keepdims=True), axis=0, keepdims=True)
        late = jnp.where(lane == phase, wrong, late)
    return picks.astype(jnp.int32), source * most + turn, late


def exchange_kernel(n_data, n_tensor, per_rank, turns, starts_ref, table_ref, embed_ref, head_ref,
                    incoming_ref, again_ref, again_second_ref, where_ref, late_ref,
                    offsets_ref, table, notes, picks, rows, trail, near, shallow, far, ready, second, rest, patched, patched_second,
                    load_sems, note_sems, save_sem, keep_sems, edge_send, edge_recv, send_sems, recv_sems):
    data, rank = lax.axis_index("dp"), lax.axis_index("tensor")
    devices = n_data * n_tensor
    me = data * n_tensor + rank
    span = per_rank * BLOCK
    height = rows.shape[1] * TILE
    edge = trail.shape[1]
    most = incoming_ref.shape[0] // devices
    cut = shallow.shape[1]
    groups = LANES // (most * n_tensor)
    even = rank % 2 == 0
    near_rank = jnp.where(even, rank + 1, rank - 1)
    far_rank = jnp.where(even, (rank + n_tensor - 1) % n_tensor, (rank + 1) % n_tensor)
    left = (rank + n_tensor - 1) % n_tensor

    loads = [
        pltpu.make_async_copy(buffer, rows.at[m], load_sems.at[m])
        for m, buffer in enumerate((embed_ref, head_ref))
    ]
    read = pltpu.make_async_copy(table_ref, table, note_sems.at[0])
    read.start()
    starts = pltpu.make_async_copy(starts_ref, offsets_ref, note_sems.at[1])
    starts.start()
    for load in loads:
        load.start()

    def peer(k):
        return (data + k % n_data) % n_data, (rank + k // n_data) % n_tensor

    barrier = pltpu.get_barrier_semaphore()

    def greet(k, carry):
        d, t = peer(k)
        pl.semaphore_signal(barrier, inc=1, device_id=(d, t), device_id_type=MESH)
        return carry

    lax.fori_loop(1, devices, greet, 0)

    read.wait()
    starts.wait()
    found = plan(rank, n_tensor, per_rank, most * n_tensor, turns, offsets_ref, table[...])
    for i in range(3):
        notes[i] = found[i]
    for load in loads:
        load.wait()

    def fill(i, carry):
        for m in range(2):
            trail[m, i] = rows[m, tile_of(tail_begin(offsets_ref[m, rank], rank, span, height)) + i]
        return carry

    lax.fori_loop(0, edge, fill, 0)
    note = pltpu.make_async_copy(notes, picks, note_sems.at[0])
    note.start()
    pass_on = pltpu.make_async_copy(notes.at[1], where_ref, note_sems.at[1])
    pass_on.start()
    pl.semaphore_wait(barrier, devices - 1)

    def edge_copy(source, target, which, t):
        return pltpu.make_async_remote_copy(
            src_ref=source, dst_ref=target, send_sem=edge_send.at[which], recv_sem=edge_recv.at[which],
            device_id=(data, t), device_id_type=MESH,
        )

    whole, upper, lower = pl.ds(0, edge), pl.ds(0, cut), pl.ds(cut, edge - cut)

    @pl.when(even)
    def _():
        edge_copy(trail, near, 0, near_rank).start()
        edge_copy(rows.at[:, upper], shallow, 1, far_rank).start()
        edge_copy(rows.at[:, lower], far.at[:, lower], 2, far_rank).start()

    @pl.when(jnp.logical_not(even))
    def _():
        edge_copy(rows.at[:, whole], near, 0, near_rank).start()
        edge_copy(trail.at[:, upper], shallow, 1, far_rank).start()
        edge_copy(trail.at[:, lower], far.at[:, lower], 2, far_rank).start()

    row = lax.broadcasted_iota(jnp.int32, (BLOCK, rows.shape[3]), 0)

    def window(buffer, m, start):
        base = jnp.clip(tile_of(start), 0, buffer.shape[1] - WINDOW // TILE)
        tiles = [buffer[m, base + i] for i in range(WINDOW // TILE)]
        return jnp.concatenate(tiles, axis=0), start - base * TILE

    def gathered(dest, j, beyond):
        number = picks[0, dest // groups, dest % groups * most + j]
        m = (number >= per_rank).astype(jnp.int32)
        first = (number - m * per_rank) * BLOCK
        low = jnp.where(m == 0, offsets_ref[0, rank], offsets_ref[1, rank]) - rank * span - first
        high = jnp.where(m == 0, offsets_ref[0, rank + 1], offsets_ref[1, rank + 1]) - rank * span - first
        left_begin = tail_begin(jnp.where(m == 0, offsets_ref[0, left], offsets_ref[1, left]), left, span, height)
        own, own_offset = window(rows, m, -low)
        from_left = first + left_begin - tile_of(left_begin) * TILE
        from_right = -high
        piece, offset = window(near, m, jnp.where(even, from_right, from_left))
        if beyond is not None:
            use_far = jnp.where(even, low > 0, high < BLOCK)
            other, other_offset = window(beyond, m, jnp.where(even, from_left, from_right))
            piece = jnp.where(use_far, other, piece)
            offset = jnp.where(use_far, other_offset, offset)
        kept = moved(own_offset, own)
        patch = moved(offset, piece)
        return jnp.where((row >= low) & (row < high), kept, patch).astype(rows.dtype)

    def send(phase, staged, count, base, d, t):
        to = d * n_tensor + t
        return pltpu.make_async_remote_copy(
            src_ref=staged.at[pl.ds(to * count, count)],
            dst_ref=incoming_ref.at[pl.ds(me * most + base, count)],
            send_sem=send_sems.at[phase, to], recv_sem=recv_sems.at[phase, me],
            device_id=(d, t), device_id_type=MESH,
        )

    def keep(phase, staged, count, base):
        return pltpu.make_async_copy(
            staged.at[pl.ds(me * count, count)], incoming_ref.at[pl.ds(me * most + base, count)], keep_sems.at[phase]
        )

    edge_copies = [
        edge_copy(trail, near, 0, near_rank),
        edge_copy(trail.at[:, upper], shallow, 1, far_rank),
        edge_copy(trail.at[:, lower], far.at[:, lower], 2, far_rank),
    ]

    def phase_of(phase, staged, count, base, beyond):
        for j in range(count):
            staged[me * count + j] = gathered(me, base + j, beyond)

        def one(k, carry):
            d, t = peer(k)
            to = d * n_tensor + t
            for j in range(count):
                staged[to * count + j] = gathered(to, base + j, beyond)

            @pl.when(k > 1)
            def _():
                send(phase, staged, count, base, *peer(k - 1)).start()

            return carry

        lax.fori_loop(1, devices, one, 0)
        send(phase, staged, count, base, *peer(devices - 1)).start()
        keep(phase, staged, count, base).start()

    phases = [
        (phase, staged, count, sum(turns[:phase]), beyond)
        for phase, (staged, count, beyond) in enumerate(zip((ready, second, rest), turns, (None, shallow, far)))
        if count
    ]

    def join(i, carry):
        for m in range(2):
            far[m, i] = shallow[m, i]
        return carry

    note.wait()
    pass_on.wait()
    late_ref[0, 0] = jnp.minimum(picks[2, 0, 0], 1) + 2 * jnp.minimum(picks[2, 0, 1], 1)
    for phase in range(3):
        edge_copies[phase].wait_recv()
        if phase == 2:
            lax.fori_loop(0, cut, join, 0)
        for entry in phases:
            if entry[0] == phase:
                phase_of(*entry)

    for entry, fixed, again in zip(phases, (patched, patched_second), (again_ref, again_second_ref)):
        phase, _, count, base, _ = entry
        if phase < 2:
            def redo(to, carry, fixed=fixed, count=count, base=base):
                for j in range(count):
                    fixed[to * count + j] = gathered(to, base + j, far)
                return carry

            lax.fori_loop(0, devices, redo, 0)
            save = pltpu.make_async_copy(fixed, again, save_sem)
            save.start()
            save.wait()

    for copy in edge_copies:
        copy.wait_send()

    def finish_phase(phase, staged, count, base):
        def drain(k, carry):
            d, t = peer(k)
            send(phase, staged, count, base, d, t).wait_send()
            pltpu.make_async_remote_copy(
                src_ref=staged.at[pl.ds(me * count, count)],
                dst_ref=incoming_ref.at[pl.ds((d * n_tensor + t) * most + base, count)],
                send_sem=send_sems.at[phase, me], recv_sem=recv_sems.at[phase, d * n_tensor + t],
                device_id=(d, t), device_id_type=MESH,
            ).wait_recv()
            return carry

        lax.fori_loop(1, devices, drain, 0)
        keep(phase, staged, count, base).wait()

    for entry in phases:
        finish_phase(*entry[:4])


def finish_kernel(n_data, n_tensor, places_ref, incoming_ref, probe_ref, stored_ref, sketch_ref,
                  where_ref, slot_of, stored, sketch, place_sem, load_sems, stored_sems, sketch_sems):
    width = incoming_ref.shape[2]
    slots = stored_ref.shape[0]
    most, groups = slots // n_tensor, LANES // slots
    buffers = sketch.shape[0]
    me = lax.axis_index("dp") * n_tensor + lax.axis_index("tensor")
    places = pltpu.make_async_copy(places_ref, where_ref, place_sem)
    places.start()
    for t in range(n_tensor):
        for d in range(n_data):
            pltpu.make_async_copy(
                incoming_ref.at[pl.ds((d * n_tensor + t) * most, most)],
                stored.at[t, :, :, pl.ds(d * width, width)],
                load_sems.at[t, d],
            ).start()
    places.wait()
    for s in range(slots):
        slot_of[where_ref[me // groups, me % groups * slots + s]] = s

    def writes(t):
        b = t % buffers
        copies = []
        for r in range(most):
            slot = slot_of[t * most + r]
            copies.append(pltpu.make_async_copy(sketch.at[b, r], sketch_ref.at[slot], sketch_sems.at[b, r]))
            copies.append(pltpu.make_async_copy(stored.at[t, r], stored_ref.at[slot], stored_sems.at[t, r]))
        return copies

    for t in range(n_tensor):
        b = t % buffers
        for d in range(n_data):
            pltpu.make_async_copy(
                incoming_ref.at[pl.ds((d * n_tensor + t) * most, most)],
                stored.at[t, :, :, pl.ds(d * width, width)],
                load_sems.at[t, d],
            ).wait()
        if t >= buffers:
            for write in writes(t - buffers):
                write.wait()
        rows = stored[t].reshape(most * BLOCK, n_data * width)
        product = jnp.dot(rows, probe_ref[...], preferred_element_type=jnp.float32)
        sketch[b] = product.reshape(sketch.shape[1:])
        for write in writes(t):
            write.start()
    for t in range(max(n_tensor - buffers, 0), n_tensor):
        for write in writes(t):
            write.wait()


def patch_kernel(n_data, n_tensor, begin, count, where_ref, fresh_ref, probe_ref, old_stored_ref, old_sketch_ref,
                 stored_ref, sketch_ref, stored, sketch, sems):
    width = fresh_ref.shape[2]
    slots = stored_ref.shape[0]
    most, groups = slots // n_tensor, LANES // slots
    me = lax.axis_index("dp") * n_tensor + lax.axis_index("tensor")

    def one(slot, carry):
        base = where_ref[me // groups, me % groups * slots + slot]
        turn = base % most

        @pl.when((turn >= begin) & (turn < begin + count))
        def _():
            for d in range(n_data):
                held = (base // most + d * n_tensor) * count + turn - begin
                stored[:, d * width : (d + 1) * width] = fresh_ref[held]
            sketch[...] = jnp.dot(stored[...], probe_ref[...], preferred_element_type=jnp.float32)
            writes = (
                pltpu.make_async_copy(stored, stored_ref.at[slot], sems.at[0]),
                pltpu.make_async_copy(sketch, sketch_ref.at[slot], sems.at[1]),
            )
            for write in writes:
                write.start()
            for write in writes:
                write.wait()

        return carry

    lax.fori_loop(0, slots, one, 0)


def exchange(row_offsets, table, embed_rows, head_rows, n_data, n_tensor, per_rank, most, turns):
    height, width = embed_rows.shape
    kind = embed_rows.dtype
    devices = n_data * n_tensor
    edge = per_rank * BLOCK // 4 // TILE + 1
    smem = pl.BlockSpec(memory_space=pltpu.SMEM)
    hbm = pl.BlockSpec(memory_space=pltpu.HBM)

    def blocks(count):
        return pltpu.VMEM((devices * max(count, 1), BLOCK, width), kind)

    def tiles(count):
        return pltpu.VMEM((2, count, TILE, width), kind)

    return pl.pallas_call(
        functools.partial(exchange_kernel, n_data, n_tensor, per_rank, turns),
        in_specs=[hbm, hbm, hbm, hbm],
        out_specs=[hbm, hbm, hbm, hbm, smem],
        out_shape=[
            jax.ShapeDtypeStruct((devices * most, BLOCK, width), kind),
            jax.ShapeDtypeStruct((devices * max(turns[0], 1), BLOCK, width), kind),
            jax.ShapeDtypeStruct((devices * max(turns[1], 1), BLOCK, width), kind),
            jax.ShapeDtypeStruct(table.shape, jnp.int32),
            jax.ShapeDtypeStruct((1, 1), jnp.int32),
        ],
        scratch_shapes=[
            pltpu.SMEM(row_offsets.shape, jnp.int32),
            pltpu.VMEM(table.shape, jnp.int32),
            pltpu.VMEM((3,) + table.shape, jnp.int32),
            pltpu.SMEM((3,) + table.shape, jnp.int32),
            tiles(height // TILE),
            tiles(edge),
            tiles(edge),
            tiles(shallow_tiles(per_rank * BLOCK)),
            tiles(edge),
            blocks(turns[0]),
            blocks(turns[1]),
            blocks(turns[2]),
            blocks(turns[0]),
            blocks(turns[1]),
            pltpu.SemaphoreType.DMA((2,)),
            pltpu.SemaphoreType.DMA((2,)),
            pltpu.SemaphoreType.DMA,
            pltpu.SemaphoreType.DMA((3,)),
            pltpu.SemaphoreType.DMA((3,)),
            pltpu.SemaphoreType.DMA((3,)),
            pltpu.SemaphoreType.DMA((3, devices)),
            pltpu.SemaphoreType.DMA((3, devices)),
        ],
        compiler_params=pltpu.CompilerParams(
            collective_id=0, has_side_effects=True, vmem_limit_bytes=57 * MIB
        ),
        name="exchange",
    )(row_offsets, table, embed_rows.reshape(-1, TILE, width), head_rows.reshape(-1, TILE, width))


def finish(where, incoming, probe, n_data, n_tensor):
    columns, sketch_width = probe.shape
    kind = incoming.dtype
    slots = incoming.shape[0] // n_data
    most = slots // n_tensor
    buffers = 3
    vmem = pl.BlockSpec(memory_space=pltpu.VMEM)
    hbm = pl.BlockSpec(memory_space=pltpu.HBM)
    return pl.pallas_call(
        functools.partial(finish_kernel, n_data, n_tensor),
        in_specs=[hbm, hbm, vmem],
        out_specs=[hbm, hbm],
        out_shape=[
            jax.ShapeDtypeStruct((slots, BLOCK, columns), kind),
            jax.ShapeDtypeStruct((slots, BLOCK, sketch_width), jnp.float32),
        ],
        scratch_shapes=[
            pltpu.SMEM(where.shape, jnp.int32),
            pltpu.SMEM((slots,), jnp.int32),
            pltpu.VMEM((n_tensor, most, BLOCK, columns), kind),
            pltpu.VMEM((buffers, most, BLOCK, sketch_width), jnp.float32),
            pltpu.SemaphoreType.DMA,
            pltpu.SemaphoreType.DMA((n_tensor, n_data)),
            pltpu.SemaphoreType.DMA((n_tensor, most)),
            pltpu.SemaphoreType.DMA((buffers, most)),
        ],
        compiler_params=pltpu.CompilerParams(vmem_limit_bytes=57 * MIB),
        name="finish",
    )(where, incoming, probe)


def patch(where, fresh, probe, stored, sketch, n_data, n_tensor, begin, count):
    smem = pl.BlockSpec(memory_space=pltpu.SMEM)
    vmem = pl.BlockSpec(memory_space=pltpu.VMEM)
    hbm = pl.BlockSpec(memory_space=pltpu.HBM)
    return pl.pallas_call(
        functools.partial(patch_kernel, n_data, n_tensor, begin, count),
        in_specs=[smem, vmem, vmem, hbm, hbm],
        out_specs=[hbm, hbm],
        out_shape=[
            jax.ShapeDtypeStruct(stored.shape, stored.dtype),
            jax.ShapeDtypeStruct(sketch.shape, sketch.dtype),
        ],
        scratch_shapes=[
            pltpu.VMEM(stored.shape[1:], stored.dtype),
            pltpu.VMEM(sketch.shape[1:], sketch.dtype),
            pltpu.SemaphoreType.DMA((2,)),
        ],
        input_output_aliases={3: 0, 4: 1},
        compiler_params=pltpu.CompilerParams(vmem_limit_bytes=32 * MIB),
        name="patch",
    )(where, fresh, probe, stored, sketch)


def shards(embed_rows, head_rows, row_offsets, slot_table, probe):
    n_data, n_tensor = lax.axis_size("dp"), lax.axis_size("tensor")
    devices = n_data * n_tensor
    per_rank = slot_table.shape[0] // (2 * n_tensor)
    slots = slot_table.shape[0] // devices
    most = slots // n_tensor
    turns = (most // 4, most // 4, most - 2 * (most // 4))
    incoming, first, second, where, late = exchange(
        row_offsets, slot_table.reshape(-1, LANES), embed_rows, head_rows, n_data, n_tensor, per_rank, most, turns
    )
    again = (first, second)
    result = tuple(finish(where, incoming, probe, n_data, n_tensor))

    def kept(where, again, probe, result):
        return result

    def resent(begin, count, phase, where, again, probe, result):
        fresh = lax.all_to_all(again[phase], AXES, split_axis=0, concat_axis=0, tiled=True)
        return tuple(patch(where, fresh, probe, *result, n_data, n_tensor, begin, count))

    def both(*args):
        return redone[1](*args[:-1], redone[0](*args))

    redone = [
        functools.partial(resent, sum(turns[:phase]), turns[phase], phase) for phase in range(2)
    ]
    if not turns[0]:
        return result
    return lax.switch(late[0, 0], [kept, *redone, both], where, again, probe, result)


def solution(mesh):
    return jax.shard_map(
        shards,
        mesh=mesh,
        in_specs=(P("tensor", "dp"), P("tensor", "dp"), P(), P(), P()),
        out_specs=(P(AXES, None, None), P(AXES, None, None)),
        check_vma=False,
    )
```
